512 devices in a mesh: seq: 16 (over z_lo, x), dp: 32 (over z_hi, y, core).
Axes of the slice: x: 4, y: 8, z: 8 (z_hi: 2, z_lo: 4; z = z_hi * 4 + z_lo), core: 2. Of those that a mesh axis runs over, the one named last changes fastest.
Arguments:
- inputs: bfloat16 [32, 3072, 2048], P('dp', 'seq'), may hold values from -6 to 6
- queries: bfloat16 [32, 3072, 2048], P('dp', 'seq'), may hold values from -6 to 6
- keys: bfloat16 [32, 3072, 512], P('dp', 'seq'), may hold values from -6 to 6
- value_matrix: bfloat16 [2048, 512], P('dp'), may hold values from -0.125 to 0.125
- out_grad: bfloat16 [32, 3072, 2048], P('dp', 'seq'), may hold values from -6 to 6
Outputs:
- query_gradient: bfloat16 [32, 3072, 2048], P('dp', 'seq')
- key_gradient: bfloat16 [32, 3072, 512], P('dp', 'seq')
- input_grad: bfloat16 [32, 3072, 2048], P('dp', 'seq')
- weight_grad: float32 [2048, 512], P('dp')
The draws below stay inside these ranges and needn't reach their ends.
All inputs are finite; a program needn't handle non-finite values.
Results may differ from the reference program's by a relative error of at most 0.0058.
Values may be sent and summed in bfloat16 or wider, within the bound.
A program may use at most 64 MiB of HBM per device.

```python
import math
from functools import partial
import jax
import jax.numpy as jnp
from jax import lax

MODEL_WIDTH = 2048
QUERY_HEADS = 32
KEY_VALUE_HEADS = 8
HEAD_WIDTH = 64
TOKENS_PER_SHARD = 192
BATCH_COUNT = 32
SEQUENCE_LENGTH = 3072


def spiked(result, rng, source, target, parts, factor):
    owner, partner = [(jnp.arange(result.shape[axis_at]) // (result.shape[axis_at] // parts)).reshape([-1 if axis == axis_at else 1 for axis in range(result.ndim)]) for axis_at in (source, target)]
    chosen = jax.random.permutation(rng, parts)[partner]
    strong = (owner == chosen) | (owner == (partner + parts // 2) % parts)
    return jnp.where(strong, factor * result, result)


def shard_levels(own_key, extent, cuts, smallest, high):
    loudness, own = 1.0, jax.random.fold_in(own_key, 6)
    for axis_at, shards_of in cuts:
        heights = jnp.exp(jax.random.uniform(jax.random.fold_in(own, axis_at), (shards_of,), jnp.float32, smallest / len(cuts), high / len(cuts)))
        loudness = loudness * jnp.repeat(heights, extent[axis_at] // shards_of).reshape([-1 if axis == axis_at else 1 for axis in range(len(extent))])
    return loudness


def gaussian(key, dims, deviation, bound, pieces=(), kind=jnp.bfloat16):
    values = jax.random.normal(key, dims, jnp.float32) * deviation
    if len(pieces) > 0:
        values = shard_levels(key, dims, pieces, -0.22, 0.18) * values
    return jnp.clip(values, min=-bound, max=bound).astype(kind)


def noise_with(stream_key, shape, deviation, bound, shards, heavy, kind=jnp.bfloat16):
    drawn = deviation * jax.random.normal(stream_key, shape, jnp.float32)
    if shards:
        drawn = drawn * shard_levels(stream_key, shape, shards, -0.22, 0.18)
    return jnp.clip(spiked(drawn, jax.random.fold_in(stream_key, 3), *heavy), -bound, bound).astype(kind)


def setup_inputs(seed: int = 0) -> dict:
    seeds = jax.random.split(jax.random.key(seed), 6)
    inputs = noise_with(seeds[0], (BATCH_COUNT, SEQUENCE_LENGTH, MODEL_WIDTH), 1.0, 6.0, ((0, 32), (1, 16)), (0, 2, 32, 2.75))
    queries = gaussian(seeds[1], (BATCH_COUNT, SEQUENCE_LENGTH, QUERY_HEADS * HEAD_WIDTH), 1.0, 6.0, ((0, 32), (1, 16)))
    keys = gaussian(seeds[2], (BATCH_COUNT, SEQUENCE_LENGTH, KEY_VALUE_HEADS * HEAD_WIDTH), 1.0, 6.0, ((0, 32), (1, 16)))
    value_matrix = gaussian(seeds[3], (MODEL_WIDTH, KEY_VALUE_HEADS * HEAD_WIDTH), MODEL_WIDTH ** -0.5, 0.125, ((0, 32),))
    out_grad = gaussian(seeds[4], (BATCH_COUNT, SEQUENCE_LENGTH, QUERY_HEADS * HEAD_WIDTH), 1.0, 6.0, ((0, 32), (1, 16)))
    return dict(inputs=inputs, queries=queries, keys=keys, value_matrix=value_matrix, out_grad=out_grad)


def one_sequence(operands, value_matrix):
    inputs, queries, keys, out_grad = operands
    highest = lax.Precision.HIGHEST
    group_width = QUERY_HEADS // KEY_VALUE_HEADS
    block_list = SEQUENCE_LENGTH // TOKENS_PER_SHARD
    value_tensor = jnp.dot(inputs, value_matrix, preferred_element_type=jnp.float32).astype(jnp.bfloat16)
    position = jnp.arange(SEQUENCE_LENGTH, dtype=jnp.int32)
    row_scale = lax.rsqrt((position.astype(jnp.float32) + 1.0) * HEAD_WIDTH)
    scaled_output = (out_grad.astype(jnp.float32) * row_scale[:, None]).astype(jnp.bfloat16)
    query_wide = queries.astype(jnp.float32).reshape(block_list, TOKENS_PER_SHARD, KEY_VALUE_HEADS, group_width, HEAD_WIDTH)
    scaled_wide = scaled_output.astype(jnp.float32).reshape(block_list, TOKENS_PER_SHARD, KEY_VALUE_HEADS, group_width, HEAD_WIDTH)
    keys_wide = keys.astype(jnp.float32).reshape(block_list, TOKENS_PER_SHARD, KEY_VALUE_HEADS, HEAD_WIDTH)
    values_wide = value_tensor.astype(jnp.float32).reshape(block_list, TOKENS_PER_SHARD, KEY_VALUE_HEADS, HEAD_WIDTH)
    key_state = jnp.einsum('ntgd,ntge->ngde', keys_wide, values_wide, precision=highest)
    prefix = jnp.cumsum(key_state, 0) - key_state
    query_state = jnp.einsum('ntghd,ntghe->ngde', query_wide, scaled_wide, precision=highest)
    suffix = lax.optimization_barrier(jnp.sum(query_state, 0, keepdims=True)) - jnp.cumsum(query_state, 0)
    causal = jnp.arange(TOKENS_PER_SHARD)[:, None] >= jnp.arange(TOKENS_PER_SHARD)[None, :]
    value_scores = jnp.where(causal, jnp.einsum('ntghe,nsge->nghts', scaled_wide, values_wide, precision=highest), 0.0)
    key_scores = jnp.where(causal, jnp.einsum('ntghd,nsgd->nghts', query_wide, keys_wide, precision=highest), 0.0)
    query_gradient = jnp.einsum('nghts,nsgd->ntghd', value_scores, keys_wide, precision=highest)
    query_gradient = query_gradient + jnp.einsum('ngde,ntghe->ntghd', prefix, scaled_wide, precision=highest)
    key_gradient = jnp.einsum('nghts,ntghd->nsgd', value_scores, query_wide, precision=highest)
    key_gradient = key_gradient + jnp.einsum('ngde,nsge->nsgd', suffix, values_wide, precision=highest)
    value_gradient = jnp.einsum('nghts,ntghe->nsge', key_scores, scaled_wide, precision=highest)
    value_gradient = value_gradient + jnp.einsum('ngde,nsgd->nsge', suffix, keys_wide, precision=highest)
    return (query_gradient.astype(jnp.bfloat16).reshape(SEQUENCE_LENGTH, QUERY_HEADS * HEAD_WIDTH), key_gradient.astype(jnp.bfloat16).reshape(SEQUENCE_LENGTH, KEY_VALUE_HEADS * HEAD_WIDTH), value_gradient.astype(jnp.bfloat16).reshape(SEQUENCE_LENGTH, KEY_VALUE_HEADS * HEAD_WIDTH))

def reference(inputs, queries, keys, value_matrix, out_grad):
    query_gradient, key_gradient, value_gradient = lax.map(partial(one_sequence, value_matrix=value_matrix), (inputs, queries, keys, out_grad))
    input_grad = jnp.einsum('bsk,dk->bsd', value_gradient.astype(jnp.float32), value_matrix.astype(jnp.float32), precision=lax.Precision.HIGHEST).astype(jnp.bfloat16)
    summed_state = jnp.dot(inputs.reshape(BATCH_COUNT * SEQUENCE_LENGTH, MODEL_WIDTH).T, value_gradient.reshape(BATCH_COUNT * SEQUENCE_LENGTH, KEY_VALUE_HEADS * HEAD_WIDTH), preferred_element_type=jnp.float32)
    weight_grad = summed_state * (1.0 / math.sqrt(BATCH_COUNT * SEQUENCE_LENGTH))
    return (query_gradient, key_gradient, input_grad, weight_grad)
```

```python
import math
from types import SimpleNamespace

import jax
import jax.numpy as jnp
from jax import lax
from jax.experimental import pallas as pl
from jax.experimental.pallas import tpu as pltpu
from jax.sharding import Mesh
from jax.sharding import PartitionSpec as P

TOKENS = 192
WIDTH = 2048
KV_WIDTH = 512
HEAD_WIDTH = 64
GROUPS = 8
SEQ = ("zl", "x")
DP = ("zh", "y", "c")
AXES = ("zl", "x", "zh", "y", "c")
BF = jnp.bfloat16
F32 = jnp.float32
MESH = pl.DeviceIdType.MESH
TOKEN_COUNT = 98304

VMEM_SCRATCH = dict(
    x=((TOKENS, WIDTH), BF),
    x2=((TOKENS, WIDTH), BF),
    q=((TOKENS, WIDTH), BF),
    o=((TOKENS, WIDTH), BF),
    s=((TOKENS, WIDTH), BF),
    k=((TOKENS, KV_WIDTH), BF),
    kd=((GROUPS, TOKENS, 128), BF),
    v=((TOKENS, KV_WIDTH), BF),
    wb=((32, 64, KV_WIDTH), BF),
    vgi=((TOKENS, KV_WIDTH), F32),
    vg=((2, TOKENS, 256), BF),
    vgp=((TOKENS, 256), BF),
    bd=((4, 128, 128), BF),
    qgi=((TOKENS, WIDTH), F32),
    st_s=((2, 4, 64, 128), BF),
    st_r1=((2, 4, 64, 128), BF),
    st_t=((2, 64, 128), BF),
    st_r2=((2, 4, 64, 128), BF),
    st_o=((2, 4, 64, 128), BF),
    st_r3=((2, 4, 64, 128), BF),
    ga=((4, 8, 2, 16, 256), BF),
    a1=((3, 8, 2, 16, 256), BF),
    a2s=((8, 2, 16, 256), BF),
    a2r=((7, 2, 16, 256), BF),
    a3s=((2, 16, 256), BF),
    a3r=((7, 16, 256), BF),
    gb=((8, 2, 4, 16, 128), BF),
    b1=((7, 2, 4, 16, 128), BF),
    b2s=((4, 2, 16, 128), BF),
    b2r=((3, 2, 16, 128), BF),
    b3s=((2, 16, 128), BF),
    b3r=((7, 16, 128), BF),
    gc=((2, 4, 8, 16, 128), BF),
    c1=((7, 8, 16, 128), BF),
    c2s=((8, 16, 128), BF),
    c2r=((7, 16, 128), BF),
    c3s=((16, 128), BF),
    c3r=((3, 16, 128), BF),
    fa=((16, 256), F32),
    fb=((16, 128), F32),
    fc=((16, 128), F32),
    wga=((8, 16, 256), F32),
    wgb=((8, 16, 128), F32),
    wgc=((8, 16, 128), F32),
    qgo=((TOKENS, WIDTH), BF),
    kgo=((TOKENS, KV_WIDTH), BF),
    igo=((TOKENS, WIDTH), BF),
    wgo=((64, KV_WIDTH), F32),
)
SEM_SCRATCH = dict(
    ld=(5,),
    out=(4,),
    wd_s=(1,),
    wd_r=(1,),
    wz_s=(1,),
    wz_r=(1,),
    wr_s=(1,),
    wr_r=(2, 2, 4),
    xx_s=(1,),
    xx_r=(1,),
    vv_s=(1,),
    vv_r=(1,),
    st_ss=(2, 3),
    st_rs=(2, 3),
    rs_s=(3, 4),
    rs_r=(3, 4),
)


def dot(a, b, dims=((1,), (0,))):
    return lax.dot_general(a, b, (dims, ((), ())), preferred_element_type=F32)


def take_bytes(ref, sem):
    pltpu.make_async_copy(ref, ref, sem).wait()


def kernel(x_h, q_h, k_h, w_h, o_h, qg_h, kg_h, ig_h, wg_h, *scratch):
    r = SimpleNamespace(**dict(zip([*VMEM_SCRATCH, *SEM_SCRATCH], scratch)))
    zl, x, zh, y, c = (lax.axis_index(a) for a in AXES)
    seq = zl * 4 + x

    def turned(value, step, size):
        return lax.rem(value + step, size)

    def send(src, dst, ssem, rsem, **where):
        pltpu.make_async_remote_copy(
            src, dst, ssem, rsem, device_id=where, device_id_type=MESH
        ).start()

    loads = [
        pltpu.make_async_copy(a, b, r.ld.at[i])
        for i, (a, b) in enumerate(
            [
                (w_h, r.wb.at[zh * 16 + y * 2 + c]),
                (o_h, r.o),
                (q_h, r.q),
                (k_h, r.k),
                (x_h, r.x),
            ]
        )
    ]
    for load in loads:
        load.start()

    peers = [dict(c=1 - c)]
    for d in range(1, 4):
        peers += [dict(x=turned(x, d, 4)), dict(x=turned(x, d, 4), c=1 - c)]
        peers += [dict(zl=turned(zl, d, 4)), dict(zl=turned(zl, d, 4), c=1 - c)]
    peers += [dict(zh=1 - zh, zl=turned(zl, d, 4)) for d in range(4)]
    peers += [dict(y=turned(y, d, 8)) for d in range(1, 8)]
    barrier = pltpu.get_barrier_semaphore()
    for peer in peers:
        pl.semaphore_signal(barrier, inc=1, device_id=peer, device_id_type=MESH)

    low64 = lax.broadcasted_iota(jnp.int32, (64, 128), 1) < 64
    low_rows = lax.broadcasted_iota(jnp.int32, (TOKENS, 128), 1) < 64
    one_low = jnp.where(low_rows, 1.0, 0.0)
    half_masks = [one_low.astype(BF), (1.0 - one_low).astype(BF)]

    loads[1].wait()
    loads[2].wait()

    @pl.loop(0, 4)
    def _(p):
        position = seq * TOKENS + lax.broadcasted_iota(jnp.int32, (TOKENS, 128), 0)
        scale = lax.rsqrt((position.astype(F32) + 1.0) * HEAD_WIDTH)
        folded = []
        for g in range(2):
            total = None
            for j in range(2):
                col = pl.ds(pl.multiple_of(p * 512 + g * 256 + j * 128, 128), 128)
                tile = (r.o[:, col].astype(F32) * scale).astype(BF)
                r.s[:, col] = tile
                m = dot(r.q[:, col], tile, ((0,), (0,)))
                total = m if total is None else total + m
            both = jnp.where(low64, total[:64], total[64:])
            folded.append(both + pltpu.roll(both, 64, 1))
        r.st_s[0, p] = jnp.where(low64, folded[0], folded[1]).astype(BF)

    loads[0].wait()
    pl.semaphore_wait(barrier, len(peers))

    def state_first(i):
        for d in range(1, 4):
            xp = turned(x, d, 4)
            send(r.st_s.at[i, xp], r.st_r1.at[i, x], r.st_ss.at[i, 0], r.st_rs.at[i, 0], x=xp)
        r.st_r1[i, x] = r.st_s[i, x]

    def state_second(i):
        take_bytes(r.st_r1.at[i, pl.ds(0, 3)], r.st_rs.at[i, 0])
        total = sum(r.st_r1[i, p].astype(F32) for p in range(4))
        r.st_t[i] = total.astype(BF)
        for d in range(1, 4):
            zp = turned(zl, d, 4)
            send(r.st_t.at[i], r.st_r2.at[i, zl], r.st_ss.at[i, 1], r.st_rs.at[i, 1], zl=zp)
        r.st_r2[i, zl] = r.st_t[i]

    def state_third(i):
        take_bytes(r.st_r2.at[i, pl.ds(0, 3)], r.st_rs.at[i, 1])
        rows = jnp.zeros((64, 128), F32)
        for z in range(4):
            counts = z > zl if i == 0 else z < zl
            rows = rows + jnp.where(counts, r.st_r2[i, z].astype(F32), 0.0)
        for xp in range(4):
            value = rows
            for p in range(xp + 1, 4) if i == 0 else range(xp):
                value = value + r.st_r1[i, p].astype(F32)
            r.st_o[i, xp] = value.astype(BF)
        for d in range(1, 4):
            xp = turned(x, d, 4)
            send(r.st_o.at[i, xp], r.st_r3.at[i, x], r.st_ss.at[i, 2], r.st_rs.at[i, 2], x=xp)
        r.st_r3[i, x] = r.st_o[i, x]

    def state_wait(i):
        take_bytes(r.st_r3.at[i, pl.ds(0, 3)], r.st_rs.at[i, 2])

    state_first(0)

    def shard_at(j, y_from):
        row = zh if j == 0 else 1 - zh
        return r.wb.at[row * 16 + y_from * 2 + c]

    def to_partner(piece):
        send(piece, piece, r.wd_s.at[0], r.wd_r.at[0], c=1 - c)

    def along(way, j, step, piece):
        yp = turned(y, 1 if way == 0 else 7, 8)
        send(piece, piece, r.wr_s.at[0], r.wr_r.at[way, j, step - 1], y=yp)

    def relay(step, j, ways=(0, 1)):
        for way in ways:
            piece = shard_at(j, turned(y, 8 - step if way == 0 else step, 8))
            take_bytes(piece, r.wr_r.at[way, j, step - 1])
            if step < 3 or (step == 3 and way == j):
                along(way, j, step + 1, piece)
            to_partner(piece)

    own = shard_at(0, y)
    along(0, 0, 1, own)
    along(1, 0, 1, own)
    send(own, own, r.wz_s.at[0], r.wz_r.at[0], zh=1 - zh)
    to_partner(own)
    loads[4].wait()
    send(r.x, r.x2, r.xx_s.at[0], r.xx_r.at[0], c=1 - c)

    loads[3].wait()
    t_row = lax.broadcasted_iota(jnp.int32, (TOKENS, TOKENS), 0)
    t_col = lax.broadcasted_iota(jnp.int32, (TOKENS, TOKENS), 1)

    def doubled(pair, g):
        pair = pair.astype(F32)
        other = pltpu.roll(pair, 64, 1)
        low, high = (pair, other) if g == 0 else (other, pair)
        return jnp.where(low_rows, low, high).astype(BF)

    def folded_pair(totals):
        ends = [t + pltpu.roll(t, 64, 1) for t in totals]
        return jnp.where(low_rows, ends[0], ends[1])

    @pl.loop(0, 4)
    def _(p):
        pair_col = pl.ds(pl.multiple_of(p * 128, 128), 128)
        totals = []
        for g in range(2):
            twice = doubled(r.k[:, pair_col], g)
            r.kd[p * 2 + g] = twice
            total = None
            for j in range(2):
                col = pl.ds(pl.multiple_of(p * 512 + g * 256 + j * 128, 128), 128)
                q_tile, s_tile = r.q[:, col], r.s[:, col]
                for half in half_masks:
                    scores = dot(twice, q_tile * half, ((1,), (1,)))
                    scores = jnp.where(t_col >= t_row, scores, 0.0).astype(BF)
                    part = dot(scores, s_tile * half)
                    total = part if total is None else total + part
            totals.append(total)
        r.vgi[:, pair_col] = folded_pair(totals)

    relay(1, 0)
    state_second(0)
    take_bytes(r.wb.at[0], r.wz_r.at[0])
    other = shard_at(1, y)
    along(0, 1, 1, other)
    along(1, 1, 1, other)
    to_partner(other)
    relay(2, 0)
    relay(1, 1)
    state_third(0)
    relay(3, 0)
    state_wait(0)

    for p in range(4):
        pair = r.st_r3[0, p].astype(F32)
        block = jnp.concatenate(
            [jnp.where(low64, pair, 0.0), jnp.where(low64, 0.0, pair)], axis=0
        ).astype(BF)
        r.bd[p] = block
        cols = slice(p * 128, p * 128 + 128)
        total = r.vgi[:, cols] + dot(r.k[:, cols], block)
        r.vg[p // 2, :, (p % 2) * 128 : (p % 2) * 128 + 128] = total.astype(BF)
    send(r.vg.at[1 - c], r.vgp, r.vv_s.at[0], r.vv_r.at[0], c=1 - c)
    take_bytes(r.x2, r.xx_r.at[0])
    relay(2, 1)
    take_bytes(r.vgp, r.vv_r.at[0])

    vg_own = r.vg[c]
    vg_other = r.vgp[...]
    for zp in range(2):

        @pl.loop(0, 8)
        def _(yp):
            col = pl.ds(pl.multiple_of(zp * 1024 + yp * 128, 128), 128)
            part = dot(r.x[:, col], vg_own, ((0,), (0,)))
            part = (part + dot(r.x2[:, col], vg_other, ((0,), (0,)))).astype(BF)
            for u in range(4):
                r.ga[u, yp, zp] = part[16 * u : 16 * u + 16]
                r.gb[yp, zp, u] = part[64 + 16 * u : 80 + 16 * u, :128]
                r.gc[zp, u, yp] = part[64 + 16 * u : 80 + 16 * u, 128:]

    z_peers = [(dh, dl) for dh in range(2) for dl in range(4)][1:]
    for d in range(1, 4):
        xp = turned(x, d, 4)
        send(r.ga.at[xp], r.a1.at[d - 1], r.rs_s.at[0, 0], r.rs_r.at[0, 0], x=xp)
    for d in range(1, 8):
        yp = turned(y, d, 8)
        send(r.gb.at[yp], r.b1.at[d - 1], r.rs_s.at[1, 0], r.rs_r.at[1, 0], y=yp)
    for n, (dh, dl) in enumerate(z_peers):
        hp, lp = turned(zh, dh, 2), turned(zl, dl, 4)
        send(r.gc.at[hp, lp], r.c1.at[n], r.rs_s.at[2, 0], r.rs_r.at[2, 0], zh=hp, zl=lp)

    relay(4, 0, (0,))
    relay(3, 1)
    relay(4, 1, (1,))
    take_bytes(r.wb.at[pl.ds(0, 16)], r.wd_r.at[0])

    whole = r.wb[...].reshape(WIDTH, KV_WIDTH)
    r.v[...] = dot(r.x[...], whole).astype(BF)
    for p in range(4):
        cols = slice(p * 128, p * 128 + 128)
        m = dot(r.v[:, cols], r.k[:, cols], ((0,), (0,)))
        r.st_s[1, p] = jnp.where(low64, m[:64], m[64:]).astype(BF)
    state_first(1)

    vg_whole = jnp.concatenate([r.vg[0], r.vg[1]], axis=1)

    @pl.loop(0, 8)
    def _(n):
        rows = r.wb[pl.ds(n * 4, 4)].reshape(256, KV_WIDTH)
        col = pl.ds(pl.multiple_of(n * 256, 256), 256)
        r.igo[:, col] = dot(vg_whole, rows, ((1,), (1,))).astype(BF)

    outs = [
        pltpu.make_async_copy(a, b, r.out.at[i])
        for i, (a, b) in enumerate([(r.igo, ig_h), (r.kgo, kg_h), (r.qgo, qg_h), (r.wgo, wg_h)])
    ]
    outs[0].start()

    state_second(1)

    @pl.loop(0, 4)
    def _(p):
        pair_col = pl.ds(pl.multiple_of(p * 128, 128), 128)
        totals = []
        for g in range(2):
            v_twice = doubled(r.v[:, pair_col], g)
            k_twice = r.kd[p * 2 + g]
            total = None
            for j in range(2):
                col = pl.ds(pl.multiple_of(p * 512 + g * 256 + j * 128, 128), 128)
                q_tile, s_tile = r.q[:, col], r.s[:, col]
                grads = []
                for half in half_masks:
                    s_half = s_tile * half
                    scores = dot(s_half, v_twice, ((1,), (1,)))
                    scores = jnp.where(t_row >= t_col, scores, 0.0).astype(BF)
                    grads.append(dot(scores, k_twice))
                    scores = dot(v_twice, s_half, ((1,), (1,)))
                    scores = jnp.where(t_col >= t_row, scores, 0.0).astype(BF)
                    part = dot(scores, q_tile * half)
                    total = part if total is None else total + part
                r.qgi[:, col] = jnp.where(low_rows, grads[0], grads[1])
            totals.append(total)
        total = folded_pair(totals) + dot(r.v[:, pair_col], r.bd[p], ((1,), (1,)))
        r.kgo[:, pair_col] = total.astype(BF)

    outs[1].start()

    take_bytes(r.a1, r.rs_r.at[0, 0])

    @pl.loop(0, 8)
    def _(yp):
        total = r.ga[x, yp].astype(F32)
        for d in range(3):
            total = total + r.a1[d, yp].astype(F32)
        r.a2s[yp] = total.astype(BF)

    for d in range(1, 8):
        yp = turned(y, d, 8)
        send(r.a2s.at[yp], r.a2r.at[d - 1], r.rs_s.at[0, 1], r.rs_r.at[0, 1], y=yp)

    take_bytes(r.b1, r.rs_r.at[1, 0])
    for zp in range(2):
        for u in range(4):
            total = r.gb[y, zp, u].astype(F32)
            for d in range(7):
                total = total + r.b1[d, zp, u].astype(F32)
            r.b2s[u, zp] = total.astype(BF)
    for d in range(1, 4):
        xp = turned(x, d, 4)
        send(r.b2s.at[xp], r.b2r.at[d - 1], r.rs_s.at[1, 1], r.rs_r.at[1, 1], x=xp)

    take_bytes(r.c1, r.rs_r.at[2, 0])
    for yp in range(8):
        total = r.gc[zh, zl, yp].astype(F32)
        for d in range(7):
            total = total + r.c1[d, yp].astype(F32)
        r.c2s[yp] = total.astype(BF)
    for d in range(1, 8):
        yp = turned(y, d, 8)
        send(r.c2s.at[yp], r.c2r.at[d - 1], r.rs_s.at[2, 1], r.rs_r.at[2, 1], y=yp)

    state_third(1)

    take_bytes(r.b2r, r.rs_r.at[1, 1])
    for zp in range(2):
        total = r.b2s[x, zp].astype(F32)
        for d in range(3):
            total = total + r.b2r[d, zp].astype(F32)
        r.b3s[zp] = total.astype(BF)
    for n, (dh, dl) in enumerate(z_peers):
        hp, lp = turned(zh, dh, 2), turned(zl, dl, 4)
        send(r.b3s.at[hp], r.b3r.at[n], r.rs_s.at[1, 2], r.rs_r.at[1, 2], zh=hp, zl=lp)

    take_bytes(r.a2r, r.rs_r.at[0, 1])
    for zp in range(2):
        total = r.a2s[y, zp].astype(F32)
        for d in range(7):
            total = total + r.a2r[d, zp].astype(F32)
        r.a3s[zp] = total.astype(BF)
    for n, (dh, dl) in enumerate(z_peers):
        hp, lp = turned(zh, dh, 2), turned(zl, dl, 4)
        send(r.a3s.at[hp], r.a3r.at[n], r.rs_s.at[0, 2], r.rs_r.at[0, 2], zh=hp, zl=lp)

    take_bytes(r.c2r, r.rs_r.at[2, 1])
    total = r.c2s[y].astype(F32)
    for d in range(7):
        total = total + r.c2r[d].astype(F32)
    r.c3s[...] = total.astype(BF)
    for d in range(1, 4):
        xp = turned(x, d, 4)
        send(r.c3s, r.c3r.at[d - 1], r.rs_s.at[2, 2], r.rs_r.at[2, 2], x=xp)

    state_wait(1)

    @pl.loop(0, 4)
    def _(p):
        pair = r.st_r3[1, p].astype(F32)
        other_way = pltpu.roll(pair, 64, 1)
        for g in range(2):
            low, high = (pair, other_way) if g == 0 else (other_way, pair)
            block = jnp.concatenate(
                [jnp.where(low64, low, 0.0), jnp.where(low64, 0.0, high)], axis=0
            ).astype(BF)
            for j in range(2):
                col = pl.ds(pl.multiple_of(p * 512 + g * 256 + j * 128, 128), 128)
                r.qgo[:, col] = (r.qgi[:, col] + dot(r.s[:, col], block)).astype(BF)

    outs[2].start()

    factor = 1.0 / math.sqrt(TOKEN_COUNT)
    here_x, here_zl = c * 4 + x, c * 4 + zl

    take_bytes(r.c3r, r.rs_r.at[2, 2])
    total = r.c3s[...].astype(F32)
    for d in range(3):
        total = total + r.c3r[d].astype(F32)
    r.fc[...] = total * factor
    take_bytes(r.b3r, r.rs_r.at[1, 2])
    total = r.b3s[zh].astype(F32)
    for d in range(7):
        total = total + r.b3r[d].astype(F32)
    r.fb[...] = total * factor
    take_bytes(r.a3r, r.rs_r.at[0, 2])
    total = r.a3s[zh].astype(F32)
    for d in range(7):
        total = total + r.a3r[d].astype(F32)
    r.fa[...] = total * factor

    def spread(src, dst, part, axis, at):
        target = 0 if part == 0 else 1
        for d in range(1, 4):
            where = {axis: turned(at, d, 4), "c": target}
            send(src, dst, r.rs_s.at[part, 3], r.rs_r.at[part, 3], **where)

        @pl.when(c != target)
        def _():
            send(src, dst, r.rs_s.at[part, 3], r.rs_r.at[part, 3], c=target)

    spread(r.fa, r.wga.at[here_x], 0, "x", x)
    spread(r.fb, r.wgb.at[here_x], 1, "x", x)
    spread(r.fc, r.wgc.at[here_zl], 2, "zl", zl)

    @pl.when(c == 0)
    def _():
        r.wga[here_x] = r.fa[...]
        take_bytes(r.wga.at[pl.ds(0, 7)], r.rs_r.at[0, 3])
        for n in range(8):
            cp, u = divmod(n, 4)
            r.wgo[16 * u : 16 * u + 16, 256 * cp : 256 * cp + 256] = r.wga[n]
        take_bytes(r.wga.at[pl.ds(0, 3)], r.rs_s.at[0, 3])
        take_bytes(r.wgb.at[pl.ds(0, 4)], r.rs_s.at[1, 3])
        take_bytes(r.wgc.at[pl.ds(0, 4)], r.rs_s.at[2, 3])

    @pl.when(c == 1)
    def _():
        r.wgb[here_x] = r.fb[...]
        r.wgc[here_zl] = r.fc[...]
        take_bytes(r.wgb.at[pl.ds(0, 7)], r.rs_r.at[1, 3])
        take_bytes(r.wgc.at[pl.ds(0, 7)], r.rs_r.at[2, 3])
        for n in range(8):
            cp, u = divmod(n, 4)
            r.wgo[16 * u : 16 * u + 16, 256 * cp : 256 * cp + 128] = r.wgb[n]
            r.wgo[16 * u : 16 * u + 16, 256 * cp + 128 : 256 * cp + 256] = r.wgc[n]
        take_bytes(r.wga.at[pl.ds(0, 4)], r.rs_s.at[0, 3])
        take_bytes(r.wgb.at[pl.ds(0, 3)], r.rs_s.at[1, 3])
        take_bytes(r.wgc.at[pl.ds(0, 3)], r.rs_s.at[2, 3])

    outs[3].start()

    take_bytes(r.wb.at[pl.ds(0, 16)], r.wd_s.at[0])
    take_bytes(r.wb.at[0], r.wz_s.at[0])
    take_bytes(r.wb.at[pl.ds(0, 14)], r.wr_s.at[0])
    take_bytes(r.x, r.xx_s.at[0])
    take_bytes(r.vgp, r.vv_s.at[0])
    for i in range(2):
        for n in range(3):
            take_bytes(r.st_s.at[i, pl.ds(0, 3)], r.st_ss.at[i, n])
    sent = [
        [r.a1, r.a2r, r.a3r],
        [r.b1, r.b2r, r.b3r],
        [r.c1, r.c2r, r.c3r],
    ]
    for part in range(3):
        for n in range(3):
            take_bytes(sent[part][n], r.rs_s.at[part, n])
    for out in outs:
        out.wait()


def body(inputs, queries, keys, value_matrix, out_grad):
    anywhere = pl.BlockSpec(memory_space=pl.ANY)
    query_gradient, key_gradient, input_grad, weight_grad = pl.pallas_call(
        kernel,
        out_shape=(
            jax.ShapeDtypeStruct((TOKENS, WIDTH), BF),
            jax.ShapeDtypeStruct((TOKENS, KV_WIDTH), BF),
            jax.ShapeDtypeStruct((TOKENS, WIDTH), BF),
            jax.ShapeDtypeStruct((64, KV_WIDTH), F32),
        ),
        in_specs=[anywhere] * 5,
        out_specs=(anywhere,) * 4,
        scratch_shapes=[pltpu.VMEM(*spec) for spec in VMEM_SCRATCH.values()]
        + [pltpu.SemaphoreType.DMA(shape) for shape in SEM_SCRATCH.values()],
        compiler_params=pltpu.CompilerParams(collective_id=0, has_side_effects=True),
    )(inputs[0], queries[0], keys[0], value_matrix, out_grad[0])
    return query_gradient[None], key_gradient[None], input_grad[None], weight_grad


def solution(mesh):
    torus = Mesh(mesh.devices.reshape(4, 4, 2, 8, 2), AXES)
    wide = P(DP, SEQ, None)
    return jax.shard_map(
        body,
        mesh=torus,
        in_specs=(wide, wide, wide, P(DP, None), wide),
        out_specs=(wide, wide, wide, P(DP, None)),
        check_vma=False,
    )
```

```python
import math
from types import SimpleNamespace

import jax
import jax.numpy as jnp
from jax import lax
from jax.experimental import pallas as pl
from jax.experimental.pallas import tpu as pltpu
from jax.sharding import Mesh
from jax.sharding import PartitionSpec as P

TOKENS = 192
WIDTH = 2048
KV_WIDTH = 512
HEAD_WIDTH = 64
GROUPS = 8
SEQ = ("zl", "x")
DP = ("zh", "y", "c")
AXES = ("zl", "x", "zh", "y", "c")
BF = jnp.bfloat16
F32 = jnp.float32
MESH = pl.DeviceIdType.MESH
TOKEN_COUNT = 98304

OUTS = dict(
    qgo=((TOKENS, WIDTH), BF),
    kgo=((TOKENS, KV_WIDTH), BF),
    igo=((TOKENS, WIDTH), BF),
    wgo=((64, KV_WIDTH), F32),
)
VMEM_SCRATCH = dict(
    x=((TOKENS, WIDTH), BF),
    x2=((TOKENS, WIDTH), BF),
    q=((TOKENS, WIDTH), BF),
    o=((TOKENS, WIDTH), BF),
    s=((TOKENS, WIDTH), BF),
    k=((TOKENS, KV_WIDTH), BF),
    kd=((GROUPS, TOKENS, 128), BF),
    v=((TOKENS, KV_WIDTH), BF),
    wb=((32, 64, KV_WIDTH), BF),
    vgi=((TOKENS, KV_WIDTH), F32),
    vg=((2, TOKENS, 256), BF),
    vgp=((TOKENS, 256), BF),
    bd=((4, 128, 128), BF),
    qgi=((TOKENS, WIDTH), F32),
    xt=((WIDTH, TOKENS), BF),
    x2t=((WIDTH, TOKENS), BF),
    st_s=((2, 4, 64, 128), F32),
    st_r1=((2, 4, 64, 128), F32),
    st_t0=((64, 128), BF),
    st_t1=((64, 128), F32),
    st_r20=((4, 64, 128), BF),
    st_r21=((4, 64, 128), F32),
    st_o=((2, 4, 64, 128), BF),
    st_r3=((2, 4, 64, 128), BF),
    ga=((4, 8, 2, 16, 256), BF),
    a1=((3, 8, 2, 16, 256), BF),
    a2s=((8, 2, 16, 256), BF),
    a2r=((7, 2, 16, 256), BF),
    a3s=((2, 16, 256), BF),
    a3r=((7, 16, 256), BF),
    gb=((8, 2, 4, 16, 128), BF),
    b1=((7, 2, 4, 16, 128), BF),
    b2s=((4, 2, 16, 128), BF),
    b2r=((3, 2, 16, 128), BF),
    b3s=((2, 16, 128), BF),
    b3r=((7, 16, 128), BF),
    gc=((2, 4, 8, 16, 128), BF),
    c1=((7, 8, 16, 128), BF),
    c2s=((8, 16, 128), BF),
    c2r=((7, 16, 128), BF),
    c3s=((16, 128), BF),
    c3r=((3, 16, 128), BF),
    fa=((16, 256), F32),
    fb=((16, 128), F32),
    fc=((16, 128), F32),
    wga=((8, 16, 256), F32),
    wgb=((8, 16, 128), F32),
    wgc=((8, 16, 128), F32),
)
SEM_SCRATCH = dict(
    ld=(5,),
    wd_s=(1,),
    wd_r=(1,),
    wz_s=(1,),
    wz_r=(1,),
    wr_s=(1,),
    wr_r=(2, 2, 4),
    xx_s=(1,),
    xx_r=(1,),
    vv_s=(1,),
    vv_r=(1,),
    st_ss=(2, 3),
    st_rs=(2, 3),
    rs_s=(3, 4),
    rs_r=(3, 4),
)


def dot(a, b, dims=((1,), (0,))):
    return lax.dot_general(a, b, (dims, ((), ())), preferred_element_type=F32)


def span(start, size):
    if isinstance(start, int):
        return slice(start, start + size)
    return pl.ds(pl.multiple_of(start, 128), size)


def take_bytes(ref, sem):
    pltpu.make_async_copy(ref, ref, sem).wait()


def kernel(x_h, q_h, k_h, w_h, o_h, *rest):
    r = SimpleNamespace(**dict(zip([*OUTS, *VMEM_SCRATCH, *SEM_SCRATCH], rest)))
    zl, x, zh, y, c = (lax.axis_index(a) for a in AXES)
    seq = zl * 4 + x

    def turned(value, step, size):
        return lax.rem(value + step, size)

    def send(src, dst, ssem, rsem, **where):
        pltpu.make_async_remote_copy(
            src, dst, ssem, rsem, device_id=where, device_id_type=MESH
        ).start()

    loads = [
        pltpu.make_async_copy(a, b, r.ld.at[i])
        for i, (a, b) in enumerate(
            [
                (w_h, r.wb.at[zh * 16 + y * 2 + c]),
                (o_h, r.o),
                (q_h, r.q),
                (k_h, r.k),
                (x_h, r.x),
            ]
        )
    ]
    for load in loads:
        load.start()

    peers = [dict(c=1 - c)]
    for d in range(1, 4):
        peers += [dict(x=turned(x, d, 4)), dict(x=turned(x, d, 4), c=1 - c)]
        peers += [dict(zl=turned(zl, d, 4)), dict(zl=turned(zl, d, 4), c=1 - c)]
    peers += [dict(zh=1 - zh, zl=turned(zl, d, 4)) for d in range(4)]
    peers += [dict(y=turned(y, d, 8)) for d in range(1, 8)]
    barrier = pltpu.get_barrier_semaphore()
    for peer in peers:
        pl.semaphore_signal(barrier, inc=1, device_id=peer, device_id_type=MESH)

    low64 = lax.broadcasted_iota(jnp.int32, (64, 128), 1) < 64
    low_rows = lax.broadcasted_iota(jnp.int32, (TOKENS, 128), 1) < 64
    one_low = jnp.where(low_rows, 1.0, 0.0)
    half_masks = [one_low.astype(BF), (1.0 - one_low).astype(BF)]

    loads[1].wait()
    loads[2].wait()

    for p in range(4):
        position = seq * TOKENS + lax.broadcasted_iota(jnp.int32, (TOKENS, 128), 0)
        scale = lax.rsqrt((position.astype(F32) + 1.0) * HEAD_WIDTH)
        folded = []
        for g in range(2):
            total = None
            for j in range(2):
                col = span(p * 512 + g * 256 + j * 128, 128)
                tile = (r.o[:, col].astype(F32) * scale).astype(BF)
                r.s[:, col] = tile
                m = dot(r.q[:, col], tile, ((0,), (0,)))
                total = m if total is None else total + m
            both = jnp.where(low64, total[:64], total[64:])
            folded.append(both + pltpu.roll(both, 64, 1))
        r.st_s[0, p] = jnp.where(low64, folded[0], folded[1])

    loads[0].wait()
    pl.semaphore_wait(barrier, len(peers))

    row_sum, row_sums = (r.st_t0, r.st_t1), (r.st_r20, r.st_r21)

    def state_first(i):
        for d in range(1, 4):
            xp = turned(x, d, 4)
            send(r.st_s.at[i, xp], r.st_r1.at[i, x], r.st_ss.at[i, 0], r.st_rs.at[i, 0], x=xp)
        r.st_r1[i, x] = r.st_s[i, x]

    def state_second(i):
        take_bytes(r.st_r1.at[i, pl.ds(0, 3)], r.st_rs.at[i, 0])
        total = sum(r.st_r1[i, p] for p in range(4)).astype(row_sum[i].dtype)
        row_sum[i][...] = total
        for d in range(1, 4):
            zp = turned(zl, d, 4)
            send(row_sum[i], row_sums[i].at[zl], r.st_ss.at[i, 1], r.st_rs.at[i, 1], zl=zp)
        row_sums[i][zl] = total

    def state_third(i):
        take_bytes(row_sums[i].at[pl.ds(0, 3)], r.st_rs.at[i, 1])
        rows = jnp.zeros((64, 128), F32)
        for z in range(4):
            counts = z > zl if i == 0 else z < zl
            rows = rows + jnp.where(counts, row_sums[i][z].astype(F32), 0.0)
        for xp in range(4):
            value = rows
            for p in range(xp + 1, 4) if i == 0 else range(xp):
                value = value + r.st_r1[i, p]
            r.st_o[i, xp] = value.astype(BF)
        for d in range(1, 4):
            xp = turned(x, d, 4)
            send(r.st_o.at[i, xp], r.st_r3.at[i, x], r.st_ss.at[i, 2], r.st_rs.at[i, 2], x=xp)
        r.st_r3[i, x] = r.st_o[i, x]

    def state_wait(i):
        take_bytes(r.st_r3.at[i, pl.ds(0, 3)], r.st_rs.at[i, 2])

    state_first(0)

    def shard_at(j, y_from):
        row = zh if j == 0 else 1 - zh
        return r.wb.at[row * 16 + y_from * 2 + c]

    def to_partner(piece):
        send(piece, piece, r.wd_s.at[0], r.wd_r.at[0], c=1 - c)

    def along(way, j, step, piece):
        yp = turned(y, 1 if way == 0 else 7, 8)
        send(piece, piece, r.wr_s.at[0], r.wr_r.at[way, j, step - 1], y=yp)

    def relay(step, j, ways=(0, 1)):
        for way in ways:
            piece = shard_at(j, turned(y, 8 - step if way == 0 else step, 8))
            take_bytes(piece, r.wr_r.at[way, j, step - 1])
            if step < 3 or (step == 3 and way == j):
                along(way, j, step + 1, piece)
            to_partner(piece)

    own = shard_at(0, y)
    along(0, 0, 1, own)
    along(1, 0, 1, own)
    for edge, targets in ((3, (1, 0)), (0, (2, 3))):

        @pl.when(zl == edge)
        def _():
            for target in targets:
                send(own, own, r.wz_s.at[0], r.wz_r.at[0], zh=1 - zh, zl=target)

    to_partner(own)
    loads[4].wait()
    send(r.x, r.x2, r.xx_s.at[0], r.xx_r.at[0], c=1 - c)

    loads[3].wait()
    t_row = lax.broadcasted_iota(jnp.int32, (TOKENS, TOKENS), 0)
    t_col = lax.broadcasted_iota(jnp.int32, (TOKENS, TOKENS), 1)

    def doubled(pair, g):
        pair = pair.astype(F32)
        other = pltpu.roll(pair, 64, 1)
        low, high = (pair, other) if g == 0 else (other, pair)
        return jnp.where(low_rows, low, high).astype(BF)

    def folded_pair(totals):
        ends = [t + pltpu.roll(t, 64, 1) for t in totals]
        return jnp.where(low_rows, ends[0], ends[1])

    def key_scores(p):
        pair_col = span(p * 128, 128)
        totals = []
        for g in range(2):
            twice = doubled(r.k[:, pair_col], g)
            r.kd[p * 2 + g] = twice
            total = None
            for j in range(2):
                col = span(p * 512 + g * 256 + j * 128, 128)
                q_tile, s_tile = r.q[:, col], r.s[:, col]
                for half in half_masks:
                    scores = dot(twice, q_tile * half, ((1,), (1,)))
                    scores = jnp.where(t_col >= t_row, scores, 0.0).astype(BF)
                    part = dot(scores, s_tile * half)
                    total = part if total is None else total + part
            totals.append(total)
        r.vgi[:, pair_col] = folded_pair(totals)

    def transpose(src, dst, first, last):
        for n in range(first, last):
            rows = span(n * 128, 128)
            dst[rows, :] = src[:, rows].T

    for p in range(3):
        key_scores(p)
    state_second(0)
    key_scores(3)
    relay(1, 0)
    transpose(r.x, r.xt, 0, 16)
    take_bytes(r.wb.at[0], r.wz_r.at[0])
    other = shard_at(1, y)
    along(0, 1, 1, other)
    along(1, 1, 1, other)
    to_partner(other)
    take_bytes(r.x2, r.xx_r.at[0])
    transpose(r.x2, r.x2t, 0, 16)
    state_third(0)
    relay(2, 0)
    relay(1, 1)
    state_wait(0)

    for p in range(4):
        pair = r.st_r3[0, p].astype(F32)
        block = jnp.concatenate(
            [jnp.where(low64, pair, 0.0), jnp.where(low64, 0.0, pair)], axis=0
        ).astype(BF)
        r.bd[p] = block
        cols = slice(p * 128, p * 128 + 128)
        total = r.vgi[:, cols] + dot(r.k[:, cols], block)
        r.vg[p // 2, :, (p % 2) * 128 : (p % 2) * 128 + 128] = total.astype(BF)
    send(r.vg.at[1 - c], r.vgp, r.vv_s.at[0], r.vv_r.at[0], c=1 - c)
    take_bytes(r.vgp, r.vv_r.at[0])

    vg_own = r.vg[c]
    vg_other = r.vgp[...]
    for zp in range(2):
        for yp in range(8):
            rows = span(zp * 1024 + yp * 128, 128)
            part = (dot(r.xt[rows, :], vg_own) + dot(r.x2t[rows, :], vg_other)).astype(BF)
            for u in range(4):
                r.ga[u, yp, zp] = part[16 * u : 16 * u + 16]
                r.gb[yp, zp, u] = part[64 + 16 * u : 80 + 16 * u, :128]
                r.gc[zp, u, yp] = part[64 + 16 * u : 80 + 16 * u, 128:]

    z_peers = [(dh, dl) for dh in range(2) for dl in range(4)][1:]
    for d in range(1, 4):
        xp = turned(x, d, 4)
        send(r.ga.at[xp], r.a1.at[d - 1], r.rs_s.at[0, 0], r.rs_r.at[0, 0], x=xp)
    for n, (dh, dl) in enumerate(z_peers):
        hp, lp = turned(zh, dh, 2), turned(zl, dl, 4)
        send(r.gc.at[hp, lp], r.c1.at[n], r.rs_s.at[2, 0], r.rs_r.at[2, 0], zh=hp, zl=lp)

    relay(3, 0)
    relay(2, 1)
    relay(4, 0, (0,))
    relay(3, 1)
    for d in range(1, 8):
        yp = turned(y, d, 8)
        send(r.gb.at[yp], r.b1.at[d - 1], r.rs_s.at[1, 0], r.rs_r.at[1, 0], y=yp)
    relay(4, 1, (1,))
    take_bytes(r.wb.at[pl.ds(0, 16)], r.wd_r.at[0])

    whole = r.wb[...].reshape(WIDTH, KV_WIDTH)
    r.v[...] = dot(r.x[...], whole).astype(BF)
    for p in range(4):
        cols = slice(p * 128, p * 128 + 128)
        m = dot(r.v[:, cols], r.k[:, cols], ((0,), (0,)))
        r.st_s[1, p] = jnp.where(low64, m[:64], m[64:])
    state_first(1)

    def value_scores(p):
        pair_col = span(p * 128, 128)
        totals = []
        for g in range(2):
            v_twice = doubled(r.v[:, pair_col], g)
            k_twice = r.kd[p * 2 + g]
            total = None
            for j in range(2):
                col = span(p * 512 + g * 256 + j * 128, 128)
                q_tile, s_tile = r.q[:, col], r.s[:, col]
                grads = []
                for half in half_masks:
                    s_half = s_tile * half
                    scores = dot(s_half, v_twice, ((1,), (1,)))
                    scores = jnp.where(t_row >= t_col, scores, 0.0).astype(BF)
                    grads.append(dot(scores, k_twice))
                    scores = dot(v_twice, s_half, ((1,), (1,)))
                    scores = jnp.where(t_col >= t_row, scores, 0.0).astype(BF)
                    part = dot(scores, q_tile * half)
                    total = part if total is None else total + part
                r.qgi[:, col] = jnp.where(low_rows, grads[0], grads[1])
            totals.append(total)
        total = folded_pair(totals) + dot(r.v[:, pair_col], r.bd[p], ((1,), (1,)))
        r.kgo[:, pair_col] = total.astype(BF)

    take_bytes(r.a1, r.rs_r.at[0, 0])

    for yp in range(8):
        total = r.ga[x, yp].astype(F32)
        for d in range(3):
            total = total + r.a1[d, yp].astype(F32)
        r.a2s[yp] = total.astype(BF)

    for d in range(1, 8):
        yp = turned(y, d, 8)
        send(r.a2s.at[yp], r.a2r.at[d - 1], r.rs_s.at[0, 1], r.rs_r.at[0, 1], y=yp)

    take_bytes(r.b1, r.rs_r.at[1, 0])
    for zp in range(2):
        for u in range(4):
            total = r.gb[y, zp, u].astype(F32)
            for d in range(7):
                total = total + r.b1[d, zp, u].astype(F32)
            r.b2s[u, zp] = total.astype(BF)
    for d in range(1, 4):
        xp = turned(x, d, 4)
        send(r.b2s.at[xp], r.b2r.at[d - 1], r.rs_s.at[1, 1], r.rs_r.at[1, 1], x=xp)

    take_bytes(r.c1, r.rs_r.at[2, 0])
    for yp in range(8):
        total = r.gc[zh, zl, yp].astype(F32)
        for d in range(7):
            total = total + r.c1[d, yp].astype(F32)
        r.c2s[yp] = total.astype(BF)
    for d in range(1, 8):
        yp = turned(y, d, 8)
        send(r.c2s.at[yp], r.c2r.at[d - 1], r.rs_s.at[2, 1], r.rs_r.at[2, 1], y=yp)

    value_scores(0)
    value_scores(1)
    state_second(1)
    value_scores(2)
    value_scores(3)

    take_bytes(r.b2r, r.rs_r.at[1, 1])
    for zp in range(2):
        total = r.b2s[x, zp].astype(F32)
        for d in range(3):
            total = total + r.b2r[d, zp].astype(F32)
        r.b3s[zp] = total.astype(BF)
    for n, (dh, dl) in enumerate(z_peers):
        hp, lp = turned(zh, dh, 2), turned(zl, dl, 4)
        send(r.b3s.at[hp], r.b3r.at[n], r.rs_s.at[1, 2], r.rs_r.at[1, 2], zh=hp, zl=lp)

    take_bytes(r.a2r, r.rs_r.at[0, 1])
    for zp in range(2):
        total = r.a2s[y, zp].astype(F32)
        for d in range(7):
            total = total + r.a2r[d, zp].astype(F32)
        r.a3s[zp] = total.astype(BF)
    for n, (dh, dl) in enumerate(z_peers):
        hp, lp = turned(zh, dh, 2), turned(zl, dl, 4)
        send(r.a3s.at[hp], r.a3r.at[n], r.rs_s.at[0, 2], r.rs_r.at[0, 2], zh=hp, zl=lp)

    take_bytes(r.c2r, r.rs_r.at[2, 1])
    total = r.c2s[y].astype(F32)
    for d in range(7):
        total = total + r.c2r[d].astype(F32)
    r.c3s[...] = total.astype(BF)
    for d in range(1, 4):
        xp = turned(x, d, 4)
        send(r.c3s, r.c3r.at[d - 1], r.rs_s.at[2, 2], r.rs_r.at[2, 2], x=xp)

    vg_whole = jnp.concatenate([r.vg[0], r.vg[1]], axis=1)

    for n in range(8):
        rows = r.wb[pl.ds(n * 4, 4)].reshape(256, KV_WIDTH)
        col = span(n * 256, 256)
        r.igo[:, col] = dot(vg_whole, rows, ((1,), (1,))).astype(BF)

    state_third(1)

    factor = 1.0 / math.sqrt(TOKEN_COUNT)
    here_x, here_zl = c * 4 + x, c * 4 + zl

    take_bytes(r.c3r, r.rs_r.at[2, 2])
    total = r.c3s[...].astype(F32)
    for d in range(3):
        total = total + r.c3r[d].astype(F32)
    r.fc[...] = total * factor
    take_bytes(r.b3r, r.rs_r.at[1, 2])
    total = r.b3s[zh].astype(F32)
    for d in range(7):
        total = total + r.b3r[d].astype(F32)
    r.fb[...] = total * factor
    take_bytes(r.a3r, r.rs_r.at[0, 2])
    total = r.a3s[zh].astype(F32)
    for d in range(7):
        total = total + r.a3r[d].astype(F32)
    r.fa[...] = total * factor

    def spread(src, dst, part, axis, at):
        target = 0 if part == 0 else 1
        for d in range(1, 4):
            where = {axis: turned(at, d, 4), "c": target}
            send(src, dst, r.rs_s.at[part, 3], r.rs_r.at[part, 3], **where)

        @pl.when(c != target)
        def _():
            send(src, dst, r.rs_s.at[part, 3], r.rs_r.at[part, 3], c=target)

    spread(r.fa, r.wga.at[here_x], 0, "x", x)
    spread(r.fb, r.wgb.at[here_x], 1, "x", x)
    spread(r.fc, r.wgc.at[here_zl], 2, "zl", zl)

    state_wait(1)

    for p in range(4):
        pair = r.st_r3[1, p].astype(F32)
        other_way = pltpu.roll(pair, 64, 1)
        for g in range(2):
            low, high = (pair, other_way) if g == 0 else (other_way, pair)
            block = jnp.concatenate(
                [jnp.where(low64, low, 0.0), jnp.where(low64, 0.0, high)], axis=0
            ).astype(BF)
            for j in range(2):
                col = span(p * 512 + g * 256 + j * 128, 128)
                r.qgo[:, col] = (r.qgi[:, col] + dot(r.s[:, col], block)).astype(BF)


    @pl.when(c == 0)
    def _():
        r.wga[here_x] = r.fa[...]
        take_bytes(r.wga.at[pl.ds(0, 7)], r.rs_r.at[0, 3])
        for n in range(8):
            cp, u = divmod(n, 4)
            r.wgo[16 * u : 16 * u + 16, 256 * cp : 256 * cp + 256] = r.wga[n]
        take_bytes(r.wga.at[pl.ds(0, 3)], r.rs_s.at[0, 3])
        take_bytes(r.wgb.at[pl.ds(0, 4)], r.rs_s.at[1, 3])
        take_bytes(r.wgc.at[pl.ds(0, 4)], r.rs_s.at[2, 3])

    @pl.when(c == 1)
    def _():
        r.wgb[here_x] = r.fb[...]
        r.wgc[here_zl] = r.fc[...]
        take_bytes(r.wgb.at[pl.ds(0, 7)], r.rs_r.at[1, 3])
        take_bytes(r.wgc.at[pl.ds(0, 7)], r.rs_r.at[2, 3])
        for n in range(8):
            cp, u = divmod(n, 4)
            r.wgo[16 * u : 16 * u + 16, 256 * cp : 256 * cp + 128] = r.wgb[n]
            r.wgo[16 * u : 16 * u + 16, 256 * cp + 128 : 256 * cp + 256] = r.wgc[n]
        take_bytes(r.wga.at[pl.ds(0, 4)], r.rs_s.at[0, 3])
        take_bytes(r.wgb.at[pl.ds(0, 3)], r.rs_s.at[1, 3])
        take_bytes(r.wgc.at[pl.ds(0, 3)], r.rs_s.at[2, 3])


    take_bytes(r.wb.at[pl.ds(0, 16)], r.wd_s.at[0])

    @pl.when((zl == 0) | (zl == 3))
    def _():
        take_bytes(r.wb.at[pl.ds(0, 2)], r.wz_s.at[0])

    take_bytes(r.wb.at[pl.ds(0, 14)], r.wr_s.at[0])
    take_bytes(r.x, r.xx_s.at[0])
    take_bytes(r.vgp, r.vv_s.at[0])
    for i in range(2):
        take_bytes(r.st_s.at[i, pl.ds(0, 3)], r.st_ss.at[i, 0])
        take_bytes(row_sums[i].at[pl.ds(0, 3)], r.st_ss.at[i, 1])
        take_bytes(r.st_o.at[i, pl.ds(0, 3)], r.st_ss.at[i, 2])
    sent = [
        [r.a1, r.a2r, r.a3r],
        [r.b1, r.b2r, r.b3r],
        [r.c1, r.c2r, r.c3r],
    ]
    for part in range(3):
        for n in range(3):
            take_bytes(sent[part][n], r.rs_s.at[part, n])


def put_out(*refs):
    copies = [
        pltpu.make_async_copy(refs[i], refs[i + 4], refs[8].at[i]) for i in range(4)
    ]
    for copy in copies:
        copy.start()
    for copy in copies:
        copy.wait()


def body(inputs, queries, keys, value_matrix, out_grad):
    anywhere = pl.BlockSpec(memory_space=pl.ANY)
    in_vmem = pl.BlockSpec(memory_space=pltpu.VMEM)
    results = pl.pallas_call(
        kernel,
        out_shape=tuple(jax.ShapeDtypeStruct(*spec) for spec in OUTS.values()),
        in_specs=[pl.BlockSpec(memory_space=pltpu.HBM)] * 5,
        out_specs=(in_vmem,) * 4,
        scratch_shapes=[pltpu.VMEM(*spec) for spec in VMEM_SCRATCH.values()]
        + [pltpu.SemaphoreType.DMA(shape) for shape in SEM_SCRATCH.values()],
        compiler_params=pltpu.CompilerParams(
            collective_id=0, has_side_effects=True, vmem_limit_bytes=40 << 20
        ),
    )(
        *(
            pltpu.with_memory_space_constraint(a, pltpu.HBM)
            for a in (inputs[0], queries[0], keys[0], value_matrix, out_grad[0])
        )
    )
    query_gradient, key_gradient, input_grad, weight_grad = pl.pallas_call(
        put_out,
        out_shape=tuple(jax.ShapeDtypeStruct(*spec) for spec in OUTS.values()),
        in_specs=[in_vmem] * 4,
        out_specs=(anywhere,) * 4,
        scratch_shapes=[pltpu.SemaphoreType.DMA((4,))],
        compiler_params=pltpu.CompilerParams(vmem_limit_bytes=8 << 20),
    )(*results)
    return query_gradient[None], key_gradient[None], input_grad[None], weight_grad


def solution(mesh):
    torus = Mesh(mesh.devices.reshape(4, 4, 2, 8, 2), AXES)
    wide = P(DP, SEQ, None)
    return jax.shard_map(
        body,
        mesh=torus,
        in_specs=(wide, wide, wide, P(DP, None), wide),
        out_specs=(wide, wide, wide, P(DP, None)),
        check_vma=False,
    )
```

```python
import math
from types import SimpleNamespace

import jax
import jax.numpy as jnp
from jax import lax
from jax.experimental import pallas as pl
from jax.experimental.pallas import tpu as pltpu
from jax.sharding import Mesh
from jax.sharding import PartitionSpec as P

TOKENS = 192
WIDTH = 2048
KV_WIDTH = 512
HEAD_WIDTH = 64
GROUPS = 8
SEQ = ("zl", "x")
DP = ("zh", "y", "c")
AXES = ("zl", "x", "zh", "y", "c")
BF = jnp.bfloat16
F32 = jnp.float32
MESH = pl.DeviceIdType.MESH
TOKEN_COUNT = 98304

OUTS = dict(
    qgo=((TOKENS, WIDTH), BF),
    kgo=((TOKENS, KV_WIDTH), BF),
    igo=((TOKENS, WIDTH), BF),
    wgo=((64, KV_WIDTH), F32),
)
VMEM_SCRATCH = dict(
    x=((TOKENS, WIDTH), BF),
    x2=((TOKENS, WIDTH), BF),
    q=((TOKENS, WIDTH), BF),
    o=((TOKENS, WIDTH), BF),
    s=((TOKENS, WIDTH), BF),
    k=((TOKENS, KV_WIDTH), BF),
    kt=((KV_WIDTH, TOKENS), BF),
    v=((TOKENS, KV_WIDTH), BF),
    wb=((32, 64, KV_WIDTH), BF),
    vgi=((TOKENS, KV_WIDTH), F32),
    vg=((2, TOKENS, 256), BF),
    vgp=((TOKENS, 256), BF),
    bd=((4, 128, 128), BF),
    qgi=((TOKENS, WIDTH), F32),
    xt=((WIDTH, TOKENS), BF),
    x2t=((WIDTH, TOKENS), BF),
    st_s=((2, 4, 64, 128), F32),
    st_r1=((2, 4, 64, 128), F32),
    st_t0=((64, 128), BF),
    st_t1=((64, 128), BF),
    st_r20=((4, 64, 128), BF),
    st_r21=((4, 64, 128), BF),
    st_o=((2, 4, 64, 128), BF),
    st_r3=((2, 4, 64, 128), BF),
    ga=((4, 8, 2, 16, 256), BF),
    a1=((3, 8, 2, 16, 256), BF),
    a2s=((8, 2, 16, 256), BF),
    a2r=((7, 2, 16, 256), BF),
    a3s=((2, 16, 256), BF),
    a3r=((7, 16, 256), BF),
    gb=((8, 2, 4, 16, 128), BF),
    b1=((7, 2, 4, 16, 128), BF),
    b2s=((4, 2, 16, 128), BF),
    b2r=((3, 2, 16, 128), BF),
    b3s=((2, 16, 128), BF),
    b3r=((7, 16, 128), BF),
    gc=((2, 4, 8, 16, 128), BF),
    c1=((7, 8, 16, 128), BF),
    c2s=((8, 16, 128), BF),
    c2r=((7, 16, 128), BF),
    c3s=((16, 128), BF),
    c3r=((3, 16, 128), BF),
    fa=((16, 256), F32),
    fb=((16, 128), F32),
    fc=((16, 128), F32),
    wga=((8, 16, 256), F32),
    wgb=((8, 16, 128), F32),
    wgc=((8, 16, 128), F32),
)
SEM_SCRATCH = dict(
    ld=(5,),
    wd_s=(1,),
    wd_r=(2,),
    wz_s=(1,),
    wz_r=(2,),
    wr_s=(1,),
    wr_r=(2, 2, 8),
    xx_s=(1,),
    xx_r=(1,),
    vv_s=(1,),
    vv_r=(1,),
    st_ss=(2, 3),
    st_rs=(2, 3),
    rs_s=(3, 4),
    rs_r=(3, 4),
)


def dot(a, b, dims=((1,), (0,))):
    return lax.dot_general(a, b, (dims, ((), ())), preferred_element_type=F32)


def span(start, size):
    if isinstance(start, int):
        return slice(start, start + size)
    return pl.ds(pl.multiple_of(start, 128), size)


def take_bytes(ref, sem):
    pltpu.make_async_copy(ref, ref, sem).wait()


def kernel(x_h, q_h, k_h, w_h, o_h, *rest):
    r = SimpleNamespace(**dict(zip([*OUTS, *VMEM_SCRATCH, *SEM_SCRATCH], rest)))
    zl, x, zh, y, c = (lax.axis_index(a) for a in AXES)
    seq = zl * 4 + x

    def turned(value, step, size):
        return lax.rem(value + step, size)

    def send(src, dst, ssem, rsem, **where):
        pltpu.make_async_remote_copy(
            src, dst, ssem, rsem, device_id=where, device_id_type=MESH
        ).start()

    loads = [
        pltpu.make_async_copy(a, b, r.ld.at[i])
        for i, (a, b) in enumerate(
            [
                (o_h, r.o),
                (q_h, r.q),
                (w_h, r.wb.at[zh * 16 + y * 2 + c]),
                (k_h, r.k),
                (x_h, r.x),
            ]
        )
    ]
    for load in loads:
        load.start()

    peers = [dict(c=1 - c)]
    for d in range(1, 4):
        peers += [dict(x=turned(x, d, 4)), dict(x=turned(x, d, 4), c=1 - c)]
        peers += [dict(zl=turned(zl, d, 4)), dict(zl=turned(zl, d, 4), c=1 - c)]
    peers += [dict(zh=1 - zh, zl=turned(zl, d, 4)) for d in range(4)]
    peers += [dict(y=turned(y, d, 8)) for d in range(1, 8)]
    barrier = pltpu.get_barrier_semaphore()
    for peer in peers:
        pl.semaphore_signal(barrier, inc=1, device_id=peer, device_id_type=MESH)

    low64 = lax.broadcasted_iota(jnp.int32, (64, 128), 1) < 64
    low_rows = lax.broadcasted_iota(jnp.int32, (TOKENS, 128), 1) < 64
    one_low = jnp.where(low_rows, 1.0, 0.0)
    half_masks = [one_low.astype(BF), (1.0 - one_low).astype(BF)]

    loads[0].wait()
    loads[1].wait()

    for p in range(4):
        position = seq * TOKENS + lax.broadcasted_iota(jnp.int32, (TOKENS, 128), 0)
        scale = lax.rsqrt((position.astype(F32) + 1.0) * HEAD_WIDTH)
        folded = []
        for g in range(2):
            total = None
            for j in range(2):
                col = span(p * 512 + g * 256 + j * 128, 128)
                tile = (r.o[:, col].astype(F32) * scale).astype(BF)
                r.s[:, col] = tile
                m = dot(r.q[:, col], tile, ((0,), (0,)))
                total = m if total is None else total + m
            both = jnp.where(low64, total[:64], total[64:])
            folded.append(both + pltpu.roll(both, 64, 1))
        r.st_s[0, p] = jnp.where(low64, folded[0], folded[1])

    loads[2].wait()
    pl.semaphore_wait(barrier, len(peers))

    row_sum, row_sums = (r.st_t0, r.st_t1), (r.st_r20, r.st_r21)

    def state_first(i):
        for d in range(1, 4):
            xp = turned(x, d, 4)
            send(r.st_s.at[i, xp], r.st_r1.at[i, x], r.st_ss.at[i, 0], r.st_rs.at[i, 0], x=xp)
        r.st_r1[i, x] = r.st_s[i, x]

    def state_second(i):
        take_bytes(r.st_r1.at[i, pl.ds(0, 3)], r.st_rs.at[i, 0])
        total = sum(r.st_r1[i, p] for p in range(4)).astype(row_sum[i].dtype)
        row_sum[i][...] = total
        for d in range(1, 4):
            zp = turned(zl, d, 4)
            send(row_sum[i], row_sums[i].at[zl], r.st_ss.at[i, 1], r.st_rs.at[i, 1], zl=zp)
        row_sums[i][zl] = total

    def state_third(i):
        take_bytes(row_sums[i].at[pl.ds(0, 3)], r.st_rs.at[i, 1])
        rows = jnp.zeros((64, 128), F32)
        for z in range(4):
            counts = z > zl if i == 0 else z < zl
            rows = rows + jnp.where(counts, row_sums[i][z].astype(F32), 0.0)
        for xp in range(4):
            value = rows
            for p in range(xp + 1, 4) if i == 0 else range(xp):
                value = value + r.st_r1[i, p]
            r.st_o[i, xp] = value.astype(BF)
        for d in range(1, 4):
            xp = turned(x, d, 4)
            send(r.st_o.at[i, xp], r.st_r3.at[i, x], r.st_ss.at[i, 2], r.st_rs.at[i, 2], x=xp)
        r.st_r3[i, x] = r.st_o[i, x]

    def state_wait(i):
        take_bytes(r.st_r3.at[i, pl.ds(0, 3)], r.st_rs.at[i, 2])

    state_first(0)

    def shard_at(j, y_from, h):
        row = zh if j == 0 else 1 - zh
        return r.wb.at[row * 16 + y_from * 2 + c, pl.ds(h * 32, 32)]

    def to_partner(j, piece):
        send(piece, piece, r.wd_s.at[0], r.wd_r.at[j], c=1 - c)

    def along(way, j, step, h, piece, hops=1):
        yp = turned(y, hops if way == 0 else 8 - hops, 8)
        send(piece, piece, r.wr_s.at[0], r.wr_r.at[way, j, step - 1 + 4 * h], y=yp)

    def begin(j, h):
        piece = shard_at(j, y, h)
        along(0, j, 1, h, piece)
        along(1, j, 1, h, piece)
        to_partner(j, piece)

    def relay(step, j, ways=(0, 1)):
        for h in range(2):
            for way in ways:
                piece = shard_at(j, turned(y, 8 - step if way == 0 else step, 8), h)
                take_bytes(piece, r.wr_r.at[way, j, step - 1 + 4 * h])
                if step < 3:
                    along(way, j, step + 1, h, piece)
                if step == 2 and way == j:
                    along(way, j, 4, h, piece, 2)
                to_partner(j, piece)

    for edge, targets in ((3, (1, 0)), (0, (2, 3))):

        @pl.when(zl == edge)
        def _():
            for h in range(2):
                piece = shard_at(0, y, h)
                for target in targets:
                    send(piece, piece, r.wz_s.at[0], r.wz_r.at[h], zh=1 - zh, zl=target)

    begin(0, 0)
    begin(0, 1)
    loads[4].wait()
    send(r.x, r.x2, r.xx_s.at[0], r.xx_r.at[0], c=1 - c)

    loads[3].wait()
    t_row = lax.broadcasted_iota(jnp.int32, (TOKENS, TOKENS), 0)
    t_col = lax.broadcasted_iota(jnp.int32, (TOKENS, TOKENS), 1)

    def doubled(pair, g):
        pair = pair.astype(F32)
        other = pltpu.roll(pair, 64, 1)
        low, high = (pair, other) if g == 0 else (other, pair)
        return jnp.where(low_rows, low, high).astype(BF)

    def folded_pair(totals):
        ends = [t + pltpu.roll(t, 64, 1) for t in totals]
        return jnp.where(low_rows, ends[0], ends[1])

    def key_scores(p):
        pair_col = span(p * 128, 128)
        r.kt[pair_col, :] = r.k[:, pair_col].T
        totals = []
        for g in range(2):
            twice = doubled(r.k[:, pair_col], g)
            total = None
            for j in range(2):
                col = span(p * 512 + g * 256 + j * 128, 128)
                q_tile, s_tile = r.q[:, col], r.s[:, col]
                for half in half_masks:
                    scores = dot(twice, q_tile * half, ((1,), (1,)))
                    scores = jnp.where(t_col >= t_row, scores, 0.0).astype(BF)
                    part = dot(scores, s_tile * half)
                    total = part if total is None else total + part
            totals.append(total)
        r.vgi[:, pair_col] = folded_pair(totals)

    def transpose(src, dst, first, last):
        for n in range(first, last):
            rows = span(n * 128, 128)
            dst[rows, :] = src[:, rows].T

    for p in range(3):
        key_scores(p)
    state_second(0)
    relay(1, 0)
    key_scores(3)
    for h in range(2):
        take_bytes(shard_at(1, y, h), r.wz_r.at[h])
        begin(1, h)
    transpose(r.x, r.xt, 0, 16)
    relay(2, 0)
    take_bytes(r.x2, r.xx_r.at[0])
    transpose(r.x2, r.x2t, 0, 16)
    state_third(0)
    relay(1, 1)
    state_wait(0)

    for p in range(4):
        pair = r.st_r3[0, p].astype(F32)
        block = jnp.concatenate(
            [jnp.where(low64, pair, 0.0), jnp.where(low64, 0.0, pair)], axis=0
        ).astype(BF)
        r.bd[p] = block
        cols = slice(p * 128, p * 128 + 128)
        total = r.vgi[:, cols] + dot(r.k[:, cols], block)
        r.vg[p // 2, :, (p % 2) * 128 : (p % 2) * 128 + 128] = total.astype(BF)
    send(r.vg.at[1 - c], r.vgp, r.vv_s.at[0], r.vv_r.at[0], c=1 - c)
    relay(3, 0)
    take_bytes(r.vgp, r.vv_r.at[0])

    vg_own = r.vg[c]
    vg_other = r.vgp[...]
    for zp in range(2):
        for yp in range(8):
            rows = span(zp * 1024 + yp * 128, 128)
            part = (dot(r.xt[rows, :], vg_own) + dot(r.x2t[rows, :], vg_other)).astype(BF)
            for u in range(4):
                r.ga[u, yp, zp] = part[16 * u : 16 * u + 16]
                r.gb[yp, zp, u] = part[64 + 16 * u : 80 + 16 * u, :128]
                r.gc[zp, u, yp] = part[64 + 16 * u : 80 + 16 * u, 128:]

    z_peers = [(dh, dl) for dh in range(2) for dl in range(4)][1:]
    for d in range(1, 4):
        xp = turned(x, d, 4)
        send(r.ga.at[xp], r.a1.at[d - 1], r.rs_s.at[0, 0], r.rs_r.at[0, 0], x=xp)
    for n, (dh, dl) in enumerate(z_peers):
        hp, lp = turned(zh, dh, 2), turned(zl, dl, 4)
        send(r.gc.at[hp, lp], r.c1.at[n], r.rs_s.at[2, 0], r.rs_r.at[2, 0], zh=hp, zl=lp)

    relay(2, 1)
    for d in range(1, 8):
        yp = turned(y, d, 8)
        send(r.gb.at[yp], r.b1.at[d - 1], r.rs_s.at[1, 0], r.rs_r.at[1, 0], y=yp)
    relay(4, 0, (0,))
    relay(3, 1)
    relay(4, 1, (1,))

    take_bytes(r.a1, r.rs_r.at[0, 0])

    for yp in range(8):
        total = r.ga[x, yp].astype(F32)
        for d in range(3):
            total = total + r.a1[d, yp].astype(F32)
        r.a2s[yp] = total.astype(BF)

    for d in range(1, 8):
        yp = turned(y, d, 8)
        send(r.a2s.at[yp], r.a2r.at[d - 1], r.rs_s.at[0, 1], r.rs_r.at[0, 1], y=yp)

    take_bytes(r.wb.at[pl.ds(0, 8)], r.wd_r.at[0])
    take_bytes(r.wb.at[pl.ds(0, 8)], r.wd_r.at[1])
    whole = r.wb[...].reshape(WIDTH, KV_WIDTH)
    r.v[...] = dot(r.x[...], whole).astype(BF)
    for p in range(4):
        cols = slice(p * 128, p * 128 + 128)
        m = dot(r.v[:, cols], r.k[:, cols], ((0,), (0,)))
        r.st_s[1, p] = jnp.where(low64, m[:64], m[64:])
    state_first(1)

    def value_scores(p):
        pair_col = span(p * 128, 128)
        totals = []
        for g in range(2):
            v_twice = doubled(r.v[:, pair_col], g)
            k_rows = r.kt[p * 128 + g * 64 : p * 128 + g * 64 + 64, :]
            total = None
            for j in range(2):
                col = span(p * 512 + g * 256 + j * 128, 128)
                q_tile, s_tile = r.q[:, col], r.s[:, col]
                grads = []
                for half in half_masks:
                    scores = dot(v_twice, s_tile * half, ((1,), (1,)))
                    scores = jnp.where(t_col >= t_row, scores, 0.0).astype(BF)
                    grads.append(dot(k_rows, scores))
                    part = dot(scores, q_tile * half)
                    total = part if total is None else total + part
                r.qgi[:, col] = jnp.concatenate(grads, axis=0).T
            totals.append(total)
        total = folded_pair(totals) + dot(r.v[:, pair_col], r.bd[p], ((1,), (1,)))
        r.kgo[:, pair_col] = total.astype(BF)

    value_scores(0)
    take_bytes(r.b1, r.rs_r.at[1, 0])
    for zp in range(2):
        for u in range(4):
            total = r.gb[y, zp, u].astype(F32)
            for d in range(7):
                total = total + r.b1[d, zp, u].astype(F32)
            r.b2s[u, zp] = total.astype(BF)
    for d in range(1, 4):
        xp = turned(x, d, 4)
        send(r.b2s.at[xp], r.b2r.at[d - 1], r.rs_s.at[1, 1], r.rs_r.at[1, 1], x=xp)

    take_bytes(r.c1, r.rs_r.at[2, 0])
    for yp in range(8):
        total = r.gc[zh, zl, yp].astype(F32)
        for d in range(7):
            total = total + r.c1[d, yp].astype(F32)
        r.c2s[yp] = total.astype(BF)
    for d in range(1, 8):
        yp = turned(y, d, 8)
        send(r.c2s.at[yp], r.c2r.at[d - 1], r.rs_s.at[2, 1], r.rs_r.at[2, 1], y=yp)

    value_scores(1)
    state_second(1)

    take_bytes(r.a2r, r.rs_r.at[0, 1])
    for zp in range(2):
        total = r.a2s[y, zp].astype(F32)
        for d in range(7):
            total = total + r.a2r[d, zp].astype(F32)
        r.a3s[zp] = total.astype(BF)
    for n, (dh, dl) in enumerate(z_peers):
        hp, lp = turned(zh, dh, 2), turned(zl, dl, 4)
        send(r.a3s.at[hp], r.a3r.at[n], r.rs_s.at[0, 2], r.rs_r.at[0, 2], zh=hp, zl=lp)

    value_scores(2)
    take_bytes(r.b2r, r.rs_r.at[1, 1])
    for zp in range(2):
        total = r.b2s[x, zp].astype(F32)
        for d in range(3):
            total = total + r.b2r[d, zp].astype(F32)
        r.b3s[zp] = total.astype(BF)
    for n, (dh, dl) in enumerate(z_peers):
        hp, lp = turned(zh, dh, 2), turned(zl, dl, 4)
        send(r.b3s.at[hp], r.b3r.at[n], r.rs_s.at[1, 2], r.rs_r.at[1, 2], zh=hp, zl=lp)

    take_bytes(r.c2r, r.rs_r.at[2, 1])
    total = r.c2s[y].astype(F32)
    for d in range(7):
        total = total + r.c2r[d].astype(F32)
    r.c3s[...] = total.astype(BF)
    for d in range(1, 4):
        xp = turned(x, d, 4)
        send(r.c3s, r.c3r.at[d - 1], r.rs_s.at[2, 2], r.rs_r.at[2, 2], x=xp)

    value_scores(3)
    state_third(1)

    vg_whole = jnp.concatenate([r.vg[0], r.vg[1]], axis=1)

    for n in range(8):
        rows = r.wb[pl.ds(n * 4, 4)].reshape(256, KV_WIDTH)
        col = span(n * 256, 256)
        r.igo[:, col] = dot(vg_whole, rows, ((1,), (1,))).astype(BF)


    factor = 1.0 / math.sqrt(TOKEN_COUNT)
    here_x, here_zl = c * 4 + x, c * 4 + zl

    take_bytes(r.c3r, r.rs_r.at[2, 2])
    total = r.c3s[...].astype(F32)
    for d in range(3):
        total = total + r.c3r[d].astype(F32)
    r.fc[...] = total * factor
    take_bytes(r.b3r, r.rs_r.at[1, 2])
    total = r.b3s[zh].astype(F32)
    for d in range(7):
        total = total + r.b3r[d].astype(F32)
    r.fb[...] = total * factor
    take_bytes(r.a3r, r.rs_r.at[0, 2])
    total = r.a3s[zh].astype(F32)
    for d in range(7):
        total = total + r.a3r[d].astype(F32)
    r.fa[...] = total * factor

    def spread(src, dst, part, axis, at):
        target = 0 if part == 0 else 1
        for d in range(1, 4):
            where = {axis: turned(at, d, 4), "c": target}
            send(src, dst, r.rs_s.at[part, 3], r.rs_r.at[part, 3], **where)

        @pl.when(c != target)
        def _():
            send(src, dst, r.rs_s.at[part, 3], r.rs_r.at[part, 3], c=target)

    spread(r.fa, r.wga.at[here_x], 0, "x", x)
    spread(r.fb, r.wgb.at[here_x], 1, "x", x)
    spread(r.fc, r.wgc.at[here_zl], 2, "zl", zl)

    state_wait(1)

    for p in range(4):
        pair = r.st_r3[1, p].astype(F32)
        other_way = pltpu.roll(pair, 64, 1)
        for g in range(2):
            low, high = (pair, other_way) if g == 0 else (other_way, pair)
            block = jnp.concatenate(
                [jnp.where(low64, low, 0.0), jnp.where(low64, 0.0, high)], axis=0
            ).astype(BF)
            for j in range(2):
                col = span(p * 512 + g * 256 + j * 128, 128)
                r.qgo[:, col] = (r.qgi[:, col] + dot(r.s[:, col], block)).astype(BF)


    @pl.when(c == 0)
    def _():
        r.wga[here_x] = r.fa[...]
        take_bytes(r.wga.at[pl.ds(0, 7)], r.rs_r.at[0, 3])
        for n in range(8):
            cp, u = divmod(n, 4)
            r.wgo[16 * u : 16 * u + 16, 256 * cp : 256 * cp + 256] = r.wga[n]
        take_bytes(r.wga.at[pl.ds(0, 3)], r.rs_s.at[0, 3])
        take_bytes(r.wgb.at[pl.ds(0, 4)], r.rs_s.at[1, 3])
        take_bytes(r.wgc.at[pl.ds(0, 4)], r.rs_s.at[2, 3])

    @pl.when(c == 1)
    def _():
        r.wgb[here_x] = r.fb[...]
        r.wgc[here_zl] = r.fc[...]
        take_bytes(r.wgb.at[pl.ds(0, 7)], r.rs_r.at[1, 3])
        take_bytes(r.wgc.at[pl.ds(0, 7)], r.rs_r.at[2, 3])
        for n in range(8):
            cp, u = divmod(n, 4)
            r.wgo[16 * u : 16 * u + 16, 256 * cp : 256 * cp + 128] = r.wgb[n]
            r.wgo[16 * u : 16 * u + 16, 256 * cp + 128 : 256 * cp + 256] = r.wgc[n]
        take_bytes(r.wga.at[pl.ds(0, 4)], r.rs_s.at[0, 3])
        take_bytes(r.wgb.at[pl.ds(0, 3)], r.rs_s.at[1, 3])
        take_bytes(r.wgc.at[pl.ds(0, 3)], r.rs_s.at[2, 3])


    take_bytes(r.wb.at[pl.ds(0, 16)], r.wd_s.at[0])

    @pl.when((zl == 0) | (zl == 3))
    def _():
        take_bytes(r.wb.at[pl.ds(0, 2)], r.wz_s.at[0])

    take_bytes(r.wb.at[pl.ds(0, 14)], r.wr_s.at[0])
    take_bytes(r.x, r.xx_s.at[0])
    take_bytes(r.vgp, r.vv_s.at[0])
    for i in range(2):
        take_bytes(r.st_s.at[i, pl.ds(0, 3)], r.st_ss.at[i, 0])
        take_bytes(row_sums[i].at[pl.ds(0, 3)], r.st_ss.at[i, 1])
        take_bytes(r.st_o.at[i, pl.ds(0, 3)], r.st_ss.at[i, 2])
    sent = [
        [r.a1, r.a2r, r.a3r],
        [r.b1, r.b2r, r.b3r],
        [r.c1, r.c2r, r.c3r],
    ]
    for part in range(3):
        for n in range(3):
            take_bytes(sent[part][n], r.rs_s.at[part, n])


def put_out(*refs):
    copies = [
        pltpu.make_async_copy(refs[i], refs[i + 4], refs[8].at[i]) for i in range(4)
    ]
    for copy in copies:
        copy.start()
    for copy in copies:
        copy.wait()


def body(inputs, queries, keys, value_matrix, out_grad):
    anywhere = pl.BlockSpec(memory_space=pl.ANY)
    in_vmem = pl.BlockSpec(memory_space=pltpu.VMEM)
    results = pl.pallas_call(
        kernel,
        out_shape=tuple(jax.ShapeDtypeStruct(*spec) for spec in OUTS.values()),
        in_specs=[pl.BlockSpec(memory_space=pltpu.HBM)] * 5,
        out_specs=(in_vmem,) * 4,
        scratch_shapes=[pltpu.VMEM(*spec) for spec in VMEM_SCRATCH.values()]
        + [pltpu.SemaphoreType.DMA(shape) for shape in SEM_SCRATCH.values()],
        compiler_params=pltpu.CompilerParams(
            collective_id=0, has_side_effects=True, vmem_limit_bytes=40 << 20
        ),
    )(
        *(
            pltpu.with_memory_space_constraint(a, pltpu.HBM)
            for a in (inputs[0], queries[0], keys[0], value_matrix, out_grad[0])
        )
    )
    query_gradient, key_gradient, input_grad, weight_grad = pl.pallas_call(
        put_out,
        out_shape=tuple(jax.ShapeDtypeStruct(*spec) for spec in OUTS.values()),
        in_specs=[in_vmem] * 4,
        out_specs=(anywhere,) * 4,
        scratch_shapes=[pltpu.SemaphoreType.DMA((4,))],
        compiler_params=pltpu.CompilerParams(vmem_limit_bytes=8 << 20),
    )(*results)
    return query_gradient[None], key_gradient[None], input_grad[None], weight_grad


def solution(mesh):
    torus = Mesh(mesh.devices.reshape(4, 4, 2, 8, 2), AXES)
    wide = P(DP, SEQ, None)
    return jax.shard_map(
        body,
        mesh=torus,
        in_specs=(wide, wide, wide, P(DP, None), wide),
        out_specs=(wide, wide, wide, P(DP, None)),
        check_vma=False,
    )
```

```python
import math
from types import SimpleNamespace

import jax
import jax.numpy as jnp
from jax import lax
from jax.experimental import pallas as pl
from jax.experimental.pallas import tpu as pltpu
from jax.sharding import Mesh
from jax.sharding import PartitionSpec as P

TOKENS = 192
WIDTH = 2048
KV_WIDTH = 512
HEAD_WIDTH = 64
GROUPS = 8
SEQ = ("zl", "x")
DP = ("zh", "y", "c")
AXES = ("zl", "x", "zh", "y", "c")
BF = jnp.bfloat16
F32 = jnp.float32
MESH = pl.DeviceIdType.MESH
TOKEN_COUNT = 98304

OUTS = dict(
    qgo=((TOKENS, WIDTH), BF),
    kgo=((TOKENS, KV_WIDTH), BF),
    igo=((TOKENS, WIDTH), BF),
    wgo=((64, KV_WIDTH), F32),
)
VMEM_SCRATCH = dict(
    x=((TOKENS, WIDTH), BF),
    x2=((TOKENS, WIDTH), BF),
    q=((TOKENS, WIDTH), BF),
    o=((TOKENS, WIDTH), BF),
    s=((TOKENS, WIDTH), BF),
    k=((TOKENS, KV_WIDTH), BF),
    kt=((KV_WIDTH, TOKENS), BF),
    v=((TOKENS, KV_WIDTH), BF),
    wb=((32, 64, KV_WIDTH), BF),
    vgi=((TOKENS, KV_WIDTH), F32),
    vg=((2, TOKENS, 256), BF),
    vgp=((TOKENS, 256), BF),
    bd=((4, 128, 128), BF),
    qgi=((TOKENS, WIDTH), F32),
    xt=((WIDTH, TOKENS), BF),
    x2t=((WIDTH, TOKENS), BF),
    st_s=((2, 4, 64, 128), F32),
    st_r1=((2, 4, 64, 128), F32),
    st_t0=((64, 128), BF),
    st_t1=((64, 128), BF),
    st_r20=((4, 64, 128), BF),
    st_r21=((4, 64, 128), BF),
    st_o=((2, 4, 64, 128), BF),
    st_r3=((2, 4, 64, 128), BF),
    ga=((4, 8, 2, 16, 256), BF),
    a1=((3, 8, 2, 16, 256), BF),
    a2s=((8, 2, 16, 256), BF),
    a2r=((7, 2, 16, 256), BF),
    a3s=((2, 16, 256), BF),
    a3r=((7, 16, 256), BF),
    gb=((8, 2, 4, 16, 128), BF),
    b1=((7, 2, 4, 16, 128), BF),
    b2s=((4, 2, 16, 128), BF),
    b2r=((3, 2, 16, 128), BF),
    b3s=((2, 16, 128), BF),
    b3r=((7, 16, 128), BF),
    gc=((2, 4, 8, 16, 128), BF),
    c1=((7, 8, 16, 128), BF),
    c2s=((8, 16, 128), BF),
    c2r=((7, 16, 128), BF),
    c3s=((16, 128), BF),
    c3r=((3, 16, 128), BF),
    fa=((16, 256), F32),
    fb=((16, 128), F32),
    fc=((16, 128), F32),
    wga=((8, 16, 256), F32),
    wgb=((8, 16, 128), F32),
    wgc=((8, 16, 128), F32),
)
SEM_SCRATCH = dict(
    ld=(5,),
    wd_s=(1,),
    wd_r=(2,),
    wz_s=(1,),
    wz_r=(2,),
    wr_s=(1,),
    wr_r=(2, 2, 8),
    xx_s=(1,),
    xx_r=(1,),
    vv_s=(1,),
    vv_r=(1,),
    st_ss=(2, 3),
    st_rs=(2, 3),
    rs_s=(3, 4),
    rs_r=(3, 4),
)


def dot(a, b, dims=((1,), (0,))):
    return lax.dot_general(a, b, (dims, ((), ())), preferred_element_type=F32)


def span(start, size):
    if isinstance(start, int):
        return slice(start, start + size)
    return pl.ds(pl.multiple_of(start, 128), size)


def take_bytes(ref, sem):
    pltpu.make_async_copy(ref, ref, sem).wait()


def kernel(x_h, q_h, k_h, w_h, o_h, *rest):
    r = SimpleNamespace(**dict(zip([*OUTS, *VMEM_SCRATCH, *SEM_SCRATCH], rest)))
    zl, x, zh, y, c = (lax.axis_index(a) for a in AXES)
    seq = zl * 4 + x

    def turned(value, step, size):
        return lax.rem(value + step, size)

    def send(src, dst, ssem, rsem, **where):
        pltpu.make_async_remote_copy(
            src, dst, ssem, rsem, device_id=where, device_id_type=MESH
        ).start()

    loads = [
        pltpu.make_async_copy(a, b, r.ld.at[i])
        for i, (a, b) in enumerate(
            [
                (o_h, r.o),
                (q_h, r.q),
                (w_h, r.wb.at[zh * 16 + y * 2 + c]),
                (k_h, r.k),
                (x_h, r.x),
            ]
        )
    ]
    for load in loads:
        load.start()

    peers = [dict(c=1 - c)]
    for d in range(1, 4):
        peers += [dict(x=turned(x, d, 4)), dict(x=turned(x, d, 4), c=1 - c)]
        peers += [dict(zl=turned(zl, d, 4)), dict(zl=turned(zl, d, 4), c=1 - c)]
    peers += [dict(zh=1 - zh, zl=turned(zl, d, 4)) for d in range(4)]
    peers += [dict(y=turned(y, d, 8)) for d in range(1, 8)]
    barrier = pltpu.get_barrier_semaphore()
    for peer in peers:
        pl.semaphore_signal(barrier, inc=1, device_id=peer, device_id_type=MESH)

    low64 = lax.broadcasted_iota(jnp.int32, (64, 128), 1) < 64
    low_rows = lax.broadcasted_iota(jnp.int32, (TOKENS, 128), 1) < 64
    one_low = jnp.where(low_rows, 1.0, 0.0)
    half_masks = [one_low.astype(BF), (1.0 - one_low).astype(BF)]

    loads[0].wait()
    loads[1].wait()

    for p in range(4):
        position = seq * TOKENS + lax.broadcasted_iota(jnp.int32, (TOKENS, 128), 0)
        scale = lax.rsqrt((position.astype(F32) + 1.0) * HEAD_WIDTH)
        folded = []
        for g in range(2):
            total = None
            for j in range(2):
                col = span(p * 512 + g * 256 + j * 128, 128)
                tile = (r.o[:, col].astype(F32) * scale).astype(BF)
                r.s[:, col] = tile
                m = dot(r.q[:, col], tile, ((0,), (0,)))
                total = m if total is None else total + m
            both = jnp.where(low64, total[:64], total[64:])
            folded.append(both + pltpu.roll(both, 64, 1))
        r.st_s[0, p] = jnp.where(low64, folded[0], folded[1])

    loads[2].wait()
    pl.semaphore_wait(barrier, len(peers))

    row_sum, row_sums = (r.st_t0, r.st_t1), (r.st_r20, r.st_r21)

    def state_first(i):
        for d in range(1, 4):
            xp = turned(x, d, 4)
            send(r.st_s.at[i, xp], r.st_r1.at[i, x], r.st_ss.at[i, 0], r.st_rs.at[i, 0], x=xp)
        r.st_r1[i, x] = r.st_s[i, x]

    def state_second(i):
        take_bytes(r.st_r1.at[i, pl.ds(0, 3)], r.st_rs.at[i, 0])
        total = sum(r.st_r1[i, p] for p in range(4)).astype(row_sum[i].dtype)
        row_sum[i][...] = total
        for d in range(1, 4):
            zp = turned(zl, d, 4)
            send(row_sum[i], row_sums[i].at[zl], r.st_ss.at[i, 1], r.st_rs.at[i, 1], zl=zp)
        row_sums[i][zl] = total

    def state_third(i):
        take_bytes(row_sums[i].at[pl.ds(0, 3)], r.st_rs.at[i, 1])
        rows = jnp.zeros((64, 128), F32)
        for z in range(4):
            counts = z > zl if i == 0 else z < zl
            rows = rows + jnp.where(counts, row_sums[i][z].astype(F32), 0.0)
        for xp in range(4):
            value = rows
            for p in range(xp + 1, 4) if i == 0 else range(xp):
                value = value + r.st_r1[i, p]
            r.st_o[i, xp] = value.astype(BF)
        for d in range(1, 4):
            xp = turned(x, d, 4)
            send(r.st_o.at[i, xp], r.st_r3.at[i, x], r.st_ss.at[i, 2], r.st_rs.at[i, 2], x=xp)
        r.st_r3[i, x] = r.st_o[i, x]

    def state_wait(i):
        take_bytes(r.st_r3.at[i, pl.ds(0, 3)], r.st_rs.at[i, 2])

    state_first(0)

    def shard_at(j, y_from, h):
        row = zh if j == 0 else 1 - zh
        return r.wb.at[row * 16 + y_from * 2 + c, pl.ds(h * 32, 32)]

    def to_partner(j, piece):
        send(piece, piece, r.wd_s.at[0], r.wd_r.at[j], c=1 - c)

    def along(way, j, step, h, piece, hops=1):
        yp = turned(y, hops if way == 0 else 8 - hops, 8)
        send(piece, piece, r.wr_s.at[0], r.wr_r.at[way, j, step - 1 + 4 * h], y=yp)

    def begin(j, h):
        piece = shard_at(j, y, h)
        along(0, j, 1, h, piece)
        along(1, j, 1, h, piece)
        to_partner(j, piece)

    def relay(step, j, ways=(0, 1)):
        for h in range(2):
            for way in ways:
                piece = shard_at(j, turned(y, 8 - step if way == 0 else step, 8), h)
                take_bytes(piece, r.wr_r.at[way, j, step - 1 + 4 * h])
                if step < 3:
                    along(way, j, step + 1, h, piece)
                if step == 2 and way == j:
                    along(way, j, 4, h, piece, 2)
                to_partner(j, piece)

    for edge, targets in ((3, (1, 0)), (0, (2, 3))):

        @pl.when(zl == edge)
        def _():
            for h in range(2):
                piece = shard_at(0, y, h)
                for target in targets:
                    send(piece, piece, r.wz_s.at[0], r.wz_r.at[h], zh=1 - zh, zl=target)

    begin(0, 0)
    begin(0, 1)
    loads[4].wait()
    send(r.x, r.x2, r.xx_s.at[0], r.xx_r.at[0], c=1 - c)

    loads[3].wait()
    t_row = lax.broadcasted_iota(jnp.int32, (TOKENS, TOKENS), 0)
    t_col = lax.broadcasted_iota(jnp.int32, (TOKENS, TOKENS), 1)

    def doubled(pair, g):
        pair = pair.astype(F32)
        other = pltpu.roll(pair, 64, 1)
        low, high = (pair, other) if g == 0 else (other, pair)
        return jnp.where(low_rows, low, high).astype(BF)

    def folded_pair(totals):
        ends = [t + pltpu.roll(t, 64, 1) for t in totals]
        return jnp.where(low_rows, ends[0], ends[1])

    def key_scores(p):
        pair_col = span(p * 128, 128)
        r.kt[pair_col, :] = r.k[:, pair_col].T
        totals = []
        for g in range(2):
            twice = doubled(r.k[:, pair_col], g)
            total = None
            for j in range(2):
                col = span(p * 512 + g * 256 + j * 128, 128)
                q_tile, s_tile = r.q[:, col], r.s[:, col]
                for half in half_masks:
                    scores = dot(twice, q_tile * half, ((1,), (1,)))
                    scores = jnp.where(t_col >= t_row, scores, 0.0).astype(BF)
                    part = dot(scores, s_tile * half)
                    total = part if total is None else total + part
            totals.append(total)
        r.vgi[:, pair_col] = folded_pair(totals)

    def transpose(src, dst, first, last):
        for n in range(first, last):
            rows = span(n * 128, 128)
            dst[rows, :] = src[:, rows].T

    for p in range(3):
        key_scores(p)
    state_second(0)
    relay(1, 0)
    key_scores(3)
    for h in range(2):
        take_bytes(shard_at(1, y, h), r.wz_r.at[h])
        begin(1, h)
    transpose(r.x, r.xt, 0, 16)
    relay(2, 0)
    take_bytes(r.x2, r.xx_r.at[0])
    transpose(r.x2, r.x2t, 0, 16)
    state_third(0)
    relay(1, 1)
    state_wait(0)

    for p in range(4):
        pair = r.st_r3[0, p].astype(F32)
        block = jnp.concatenate(
            [jnp.where(low64, pair, 0.0), jnp.where(low64, 0.0, pair)], axis=0
        ).astype(BF)
        r.bd[p] = block
        cols = slice(p * 128, p * 128 + 128)
        total = r.vgi[:, cols] + dot(r.k[:, cols], block)
        r.vg[p // 2, :, (p % 2) * 128 : (p % 2) * 128 + 128] = total.astype(BF)
    send(r.vg.at[1 - c], r.vgp, r.vv_s.at[0], r.vv_r.at[0], c=1 - c)
    relay(3, 0)
    relay(2, 1)
    take_bytes(r.vgp, r.vv_r.at[0])

    vg_own = r.vg[c]
    vg_other = r.vgp[...]
    for zp in range(2):
        for yp in range(8):
            rows = span(zp * 1024 + yp * 128, 128)
            part = (dot(r.xt[rows, :], vg_own) + dot(r.x2t[rows, :], vg_other)).astype(BF)
            for u in range(4):
                r.ga[u, yp, zp] = part[16 * u : 16 * u + 16]
                r.gb[yp, zp, u] = part[64 + 16 * u : 80 + 16 * u, :128]
                r.gc[zp, u, yp] = part[64 + 16 * u : 80 + 16 * u, 128:]

    z_peers = [(dh, dl) for dh in range(2) for dl in range(4)][1:]
    for d in range(1, 4):
        xp = turned(x, d, 4)
        send(r.ga.at[xp], r.a1.at[d - 1], r.rs_s.at[0, 0], r.rs_r.at[0, 0], x=xp)
    for n, (dh, dl) in enumerate(z_peers):
        hp, lp = turned(zh, dh, 2), turned(zl, dl, 4)
        send(r.gc.at[hp, lp], r.c1.at[n], r.rs_s.at[2, 0], r.rs_r.at[2, 0], zh=hp, zl=lp)

    for d in range(1, 8):
        yp = turned(y, d, 8)
        send(r.gb.at[yp], r.b1.at[d - 1], r.rs_s.at[1, 0], r.rs_r.at[1, 0], y=yp)
    relay(4, 0, (0,))
    relay(3, 1)
    relay(4, 1, (1,))

    take_bytes(r.a1, r.rs_r.at[0, 0])

    for yp in range(8):
        total = r.ga[x, yp].astype(F32)
        for d in range(3):
            total = total + r.a1[d, yp].astype(F32)
        r.a2s[yp] = total.astype(BF)

    for d in range(1, 8):
        yp = turned(y, d, 8)
        send(r.a2s.at[yp], r.a2r.at[d - 1], r.rs_s.at[0, 1], r.rs_r.at[0, 1], y=yp)

    take_bytes(r.wb.at[pl.ds(0, 8)], r.wd_r.at[0])
    take_bytes(r.wb.at[pl.ds(0, 8)], r.wd_r.at[1])
    whole = r.wb[...].reshape(WIDTH, KV_WIDTH)
    r.v[...] = dot(r.x[...], whole).astype(BF)
    for p in range(4):
        cols = slice(p * 128, p * 128 + 128)
        m = dot(r.v[:, cols], r.k[:, cols], ((0,), (0,)))
        r.st_s[1, p] = jnp.where(low64, m[:64], m[64:])
    state_first(1)

    def value_scores(p):
        pair_col = span(p * 128, 128)
        totals = []
        for g in range(2):
            v_twice = doubled(r.v[:, pair_col], g)
            k_rows = r.kt[p * 128 + g * 64 : p * 128 + g * 64 + 64, :]
            total = None
            for j in range(2):
                col = span(p * 512 + g * 256 + j * 128, 128)
                q_tile, s_tile = r.q[:, col], r.s[:, col]
                grads = []
                for half in half_masks:
                    scores = dot(v_twice, s_tile * half, ((1,), (1,)))
                    scores = jnp.where(t_col >= t_row, scores, 0.0).astype(BF)
                    grads.append(dot(k_rows, scores))
                    part = dot(scores, q_tile * half)
                    total = part if total is None else total + part
                r.qgi[:, col] = jnp.concatenate(grads, axis=0).T
            totals.append(total)
        total = folded_pair(totals) + dot(r.v[:, pair_col], r.bd[p], ((1,), (1,)))
        r.kgo[:, pair_col] = total.astype(BF)

    value_scores(0)
    take_bytes(r.b1, r.rs_r.at[1, 0])
    for zp in range(2):
        for u in range(4):
            total = r.gb[y, zp, u].astype(F32)
            for d in range(7):
                total = total + r.b1[d, zp, u].astype(F32)
            r.b2s[u, zp] = total.astype(BF)
    for d in range(1, 4):
        xp = turned(x, d, 4)
        send(r.b2s.at[xp], r.b2r.at[d - 1], r.rs_s.at[1, 1], r.rs_r.at[1, 1], x=xp)

    take_bytes(r.c1, r.rs_r.at[2, 0])
    for yp in range(8):
        total = r.gc[zh, zl, yp].astype(F32)
        for d in range(7):
            total = total + r.c1[d, yp].astype(F32)
        r.c2s[yp] = total.astype(BF)
    for d in range(1, 8):
        yp = turned(y, d, 8)
        send(r.c2s.at[yp], r.c2r.at[d - 1], r.rs_s.at[2, 1], r.rs_r.at[2, 1], y=yp)

    value_scores(1)
    value_scores(2)
    state_second(1)

    take_bytes(r.a2r, r.rs_r.at[0, 1])
    for zp in range(2):
        total = r.a2s[y, zp].astype(F32)
        for d in range(7):
            total = total + r.a2r[d, zp].astype(F32)
        r.a3s[zp] = total.astype(BF)
    for n, (dh, dl) in enumerate(z_peers):
        hp, lp = turned(zh, dh, 2), turned(zl, dl, 4)
        send(r.a3s.at[hp], r.a3r.at[n], r.rs_s.at[0, 2], r.rs_r.at[0, 2], zh=hp, zl=lp)

    take_bytes(r.b2r, r.rs_r.at[1, 1])
    for zp in range(2):
        total = r.b2s[x, zp].astype(F32)
        for d in range(3):
            total = total + r.b2r[d, zp].astype(F32)
        r.b3s[zp] = total.astype(BF)
    for n, (dh, dl) in enumerate(z_peers):
        hp, lp = turned(zh, dh, 2), turned(zl, dl, 4)
        send(r.b3s.at[hp], r.b3r.at[n], r.rs_s.at[1, 2], r.rs_r.at[1, 2], zh=hp, zl=lp)

    take_bytes(r.c2r, r.rs_r.at[2, 1])
    total = r.c2s[y].astype(F32)
    for d in range(7):
        total = total + r.c2r[d].astype(F32)
    r.c3s[...] = total.astype(BF)
    for d in range(1, 4):
        xp = turned(x, d, 4)
        send(r.c3s, r.c3r.at[d - 1], r.rs_s.at[2, 2], r.rs_r.at[2, 2], x=xp)

    value_scores(3)
    state_third(1)

    vg_whole = jnp.concatenate([r.vg[0], r.vg[1]], axis=1)

    for n in range(8):
        rows = r.wb[pl.ds(n * 4, 4)].reshape(256, KV_WIDTH)
        col = span(n * 256, 256)
        r.igo[:, col] = dot(vg_whole, rows, ((1,), (1,))).astype(BF)


    factor = 1.0 / math.sqrt(TOKEN_COUNT)
    here_x, here_zl = c * 4 + x, c * 4 + zl

    def spread(src, dst, part, axis, at):
        target = 0 if part == 0 else 1
        for d in range(1, 4):
            where = {axis: turned(at, d, 4), "c": target}
            send(src, dst, r.rs_s.at[part, 3], r.rs_r.at[part, 3], **where)

        @pl.when(c != target)
        def _():
            send(src, dst, r.rs_s.at[part, 3], r.rs_r.at[part, 3], c=target)

    take_bytes(r.a3r, r.rs_r.at[0, 2])
    total = r.a3s[zh].astype(F32)
    for d in range(7):
        total = total + r.a3r[d].astype(F32)
    r.fa[...] = total * factor
    spread(r.fa, r.wga.at[here_x], 0, "x", x)
    take_bytes(r.c3r, r.rs_r.at[2, 2])
    total = r.c3s[...].astype(F32)
    for d in range(3):
        total = total + r.c3r[d].astype(F32)
    r.fc[...] = total * factor
    spread(r.fc, r.wgc.at[here_zl], 2, "zl", zl)
    take_bytes(r.b3r, r.rs_r.at[1, 2])
    total = r.b3s[zh].astype(F32)
    for d in range(7):
        total = total + r.b3r[d].astype(F32)
    r.fb[...] = total * factor
    spread(r.fb, r.wgb.at[here_x], 1, "x", x)

    state_wait(1)

    for p in range(4):
        pair = r.st_r3[1, p].astype(F32)
        other_way = pltpu.roll(pair, 64, 1)
        for g in range(2):
            low, high = (pair, other_way) if g == 0 else (other_way, pair)
            block = jnp.concatenate(
                [jnp.where(low64, low, 0.0), jnp.where(low64, 0.0, high)], axis=0
            ).astype(BF)
            for j in range(2):
                col = span(p * 512 + g * 256 + j * 128, 128)
                r.qgo[:, col] = (r.qgi[:, col] + dot(r.s[:, col], block)).astype(BF)


    @pl.when(c == 0)
    def _():
        r.wga[here_x] = r.fa[...]
        take_bytes(r.wga.at[pl.ds(0, 7)], r.rs_r.at[0, 3])
        for n in range(8):
            cp, u = divmod(n, 4)
            r.wgo[16 * u : 16 * u + 16, 256 * cp : 256 * cp + 256] = r.wga[n]
        take_bytes(r.wga.at[pl.ds(0, 3)], r.rs_s.at[0, 3])
        take_bytes(r.wgb.at[pl.ds(0, 4)], r.rs_s.at[1, 3])
        take_bytes(r.wgc.at[pl.ds(0, 4)], r.rs_s.at[2, 3])

    @pl.when(c == 1)
    def _():
        r.wgb[here_x] = r.fb[...]
        r.wgc[here_zl] = r.fc[...]
        take_bytes(r.wgb.at[pl.ds(0, 7)], r.rs_r.at[1, 3])
        take_bytes(r.wgc.at[pl.ds(0, 7)], r.rs_r.at[2, 3])
        for n in range(8):
            cp, u = divmod(n, 4)
            r.wgo[16 * u : 16 * u + 16, 256 * cp : 256 * cp + 128] = r.wgb[n]
            r.wgo[16 * u : 16 * u + 16, 256 * cp + 128 : 256 * cp + 256] = r.wgc[n]
        take_bytes(r.wga.at[pl.ds(0, 4)], r.rs_s.at[0, 3])
        take_bytes(r.wgb.at[pl.ds(0, 3)], r.rs_s.at[1, 3])
        take_bytes(r.wgc.at[pl.ds(0, 3)], r.rs_s.at[2, 3])


    take_bytes(r.wb.at[pl.ds(0, 16)], r.wd_s.at[0])

    @pl.when((zl == 0) | (zl == 3))
    def _():
        take_bytes(r.wb.at[pl.ds(0, 2)], r.wz_s.at[0])

    take_bytes(r.wb.at[pl.ds(0, 14)], r.wr_s.at[0])
    take_bytes(r.x, r.xx_s.at[0])
    take_bytes(r.vgp, r.vv_s.at[0])
    for i in range(2):
        take_bytes(r.st_s.at[i, pl.ds(0, 3)], r.st_ss.at[i, 0])
        take_bytes(row_sums[i].at[pl.ds(0, 3)], r.st_ss.at[i, 1])
        take_bytes(r.st_o.at[i, pl.ds(0, 3)], r.st_ss.at[i, 2])
    sent = [
        [r.a1, r.a2r, r.a3r],
        [r.b1, r.b2r, r.b3r],
        [r.c1, r.c2r, r.c3r],
    ]
    for part in range(3):
        for n in range(3):
            take_bytes(sent[part][n], r.rs_s.at[part, n])


def put_out(*refs):
    copies = [
        pltpu.make_async_copy(refs[i], refs[i + 4], refs[8].at[i]) for i in range(4)
    ]
    for copy in copies:
        copy.start()
    for copy in copies:
        copy.wait()


def body(inputs, queries, keys, value_matrix, out_grad):
    anywhere = pl.BlockSpec(memory_space=pl.ANY)
    in_vmem = pl.BlockSpec(memory_space=pltpu.VMEM)
    results = pl.pallas_call(
        kernel,
        out_shape=tuple(jax.ShapeDtypeStruct(*spec) for spec in OUTS.values()),
        in_specs=[pl.BlockSpec(memory_space=pltpu.HBM)] * 5,
        out_specs=(in_vmem,) * 4,
        scratch_shapes=[pltpu.VMEM(*spec) for spec in VMEM_SCRATCH.values()]
        + [pltpu.SemaphoreType.DMA(shape) for shape in SEM_SCRATCH.values()],
        compiler_params=pltpu.CompilerParams(
            collective_id=0, has_side_effects=True, vmem_limit_bytes=40 << 20
        ),
    )(
        *(
            pltpu.with_memory_space_constraint(a, pltpu.HBM)
            for a in (inputs[0], queries[0], keys[0], value_matrix, out_grad[0])
        )
    )
    query_gradient, key_gradient, input_grad, weight_grad = pl.pallas_call(
        put_out,
        out_shape=tuple(jax.ShapeDtypeStruct(*spec) for spec in OUTS.values()),
        in_specs=[in_vmem] * 4,
        out_specs=(anywhere,) * 4,
        scratch_shapes=[pltpu.SemaphoreType.DMA((4,))],
        compiler_params=pltpu.CompilerParams(vmem_limit_bytes=8 << 20),
    )(*results)
    return query_gradient[None], key_gradient[None], input_grad[None], weight_grad


def solution(mesh):
    torus = Mesh(mesh.devices.reshape(4, 4, 2, 8, 2), AXES)
    wide = P(DP, SEQ, None)
    return jax.shard_map(
        body,
        mesh=torus,
        in_specs=(wide, wide, wide, P(DP, None), wide),
        out_specs=(wide, wide, wide, P(DP, None)),
        check_vma=False,
    )
```

```python
import math
from types import SimpleNamespace

import jax
import jax.numpy as jnp
from jax import lax
from jax.experimental import pallas as pl
from jax.experimental.pallas import tpu as pltpu
from jax.sharding import Mesh
from jax.sharding import PartitionSpec as P

TOKENS = 192
WIDTH = 2048
KV_WIDTH = 512
HEAD_WIDTH = 64
GROUPS = 8
SEQ = ("zl", "x")
DP = ("zh", "y", "c")
AXES = ("zl", "x", "zh", "y", "c")
BF = jnp.bfloat16
F32 = jnp.float32
MESH = pl.DeviceIdType.MESH
TOKEN_COUNT = 98304
FAR_FIRST_4 = (2, 1, 3)
FAR_FIRST_8 = (4, 3, 5, 2, 6, 1, 7)

OUTS = dict(
    qgo=((TOKENS, WIDTH), BF),
    kgo=((TOKENS, KV_WIDTH), BF),
    igo=((TOKENS, WIDTH), BF),
    wgo=((64, KV_WIDTH), F32),
)
VMEM_SCRATCH = dict(
    x=((TOKENS, WIDTH), BF),
    x2=((TOKENS, WIDTH), BF),
    q=((TOKENS, WIDTH), BF),
    o=((TOKENS, WIDTH), BF),
    s=((TOKENS, WIDTH), BF),
    k=((TOKENS, KV_WIDTH), BF),
    kt=((KV_WIDTH, TOKENS), BF),
    v=((TOKENS, KV_WIDTH), BF),
    wb=((32, 64, KV_WIDTH), BF),
    vgi=((TOKENS, KV_WIDTH), F32),
    vg=((2, TOKENS, 256), BF),
    vgp=((TOKENS, 256), BF),
    bd=((4, 128, 128), BF),
    qgi=((TOKENS, WIDTH), F32),
    xt=((WIDTH, TOKENS), BF),
    x2t=((WIDTH, TOKENS), BF),
    st_s=((2, 4, 64, 128), F32),
    st_r1=((2, 4, 64, 128), F32),
    st_t0=((64, 128), BF),
    st_t1=((64, 128), BF),
    st_r20=((4, 64, 128), BF),
    st_r21=((4, 64, 128), BF),
    st_o=((2, 4, 64, 128), BF),
    st_r3=((2, 4, 64, 128), BF),
    ga=((4, 8, 2, 16, 256), BF),
    a1=((3, 8, 2, 16, 256), BF),
    a2s=((8, 2, 16, 256), BF),
    a2r=((7, 2, 16, 256), BF),
    a3s=((2, 16, 256), BF),
    a3r=((7, 16, 256), BF),
    gb=((8, 2, 4, 16, 128), BF),
    b1=((7, 2, 4, 16, 128), BF),
    b2s=((4, 2, 16, 128), BF),
    b2r=((3, 2, 16, 128), BF),
    b3s=((2, 16, 128), BF),
    b3r=((7, 16, 128), BF),
    gc=((2, 4, 8, 16, 128), BF),
    c1=((7, 8, 16, 128), BF),
    c2s=((8, 16, 128), BF),
    c2r=((7, 16, 128), BF),
    c3s=((16, 128), BF),
    c3r=((3, 16, 128), BF),
    fa=((16, 256), F32),
    fb=((16, 128), F32),
    fc=((16, 128), F32),
    wga=((8, 16, 256), F32),
    wgb=((8, 16, 128), F32),
    wgc=((8, 16, 128), F32),
)
SEM_SCRATCH = dict(
    ld=(5,),
    wd_s=(1,),
    wd_r=(2,),
    wz_s=(1,),
    wz_r=(2,),
    wr_s=(1,),
    wr_r=(2, 2, 8),
    xx_s=(1,),
    xx_r=(1,),
    vv_s=(1,),
    vv_r=(1,),
    st_ss=(2, 3),
    st_rs=(2, 3),
    rs_s=(3, 4),
    rs_r=(3, 4),
)


def dot(a, b, dims=((1,), (0,))):
    return lax.dot_general(a, b, (dims, ((), ())), preferred_element_type=F32)


def span(start, size):
    if isinstance(start, int):
        return slice(start, start + size)
    return pl.ds(pl.multiple_of(start, 128), size)


def take_bytes(ref, sem):
    pltpu.make_async_copy(ref, ref, sem).wait()


def kernel(x_h, q_h, k_h, w_h, o_h, *rest):
    r = SimpleNamespace(**dict(zip([*OUTS, *VMEM_SCRATCH, *SEM_SCRATCH], rest)))
    zl, x, zh, y, c = (lax.axis_index(a) for a in AXES)
    seq = zl * 4 + x

    def turned(value, step, size):
        return lax.rem(value + step, size)

    def send(src, dst, ssem, rsem, **where):
        pltpu.make_async_remote_copy(
            src, dst, ssem, rsem, device_id=where, device_id_type=MESH
        ).start()

    loads = [
        pltpu.make_async_copy(a, b, r.ld.at[i])
        for i, (a, b) in enumerate(
            [
                (o_h, r.o),
                (q_h, r.q),
                (w_h, r.wb.at[zh * 16 + y * 2 + c]),
                (k_h, r.k),
                (x_h, r.x),
            ]
        )
    ]
    for load in loads:
        load.start()

    peers = [dict(c=1 - c)]
    for d in range(1, 4):
        peers += [dict(x=turned(x, d, 4)), dict(x=turned(x, d, 4), c=1 - c)]
        peers += [dict(zl=turned(zl, d, 4)), dict(zl=turned(zl, d, 4), c=1 - c)]
    peers += [dict(zh=1 - zh, zl=turned(zl, d, 4)) for d in range(4)]
    peers += [dict(y=turned(y, d, 8)) for d in range(1, 8)]
    barrier = pltpu.get_barrier_semaphore()
    for peer in peers:
        pl.semaphore_signal(barrier, inc=1, device_id=peer, device_id_type=MESH)

    low64 = lax.broadcasted_iota(jnp.int32, (64, 128), 1) < 64
    low_rows = lax.broadcasted_iota(jnp.int32, (TOKENS, 128), 1) < 64
    one_low = jnp.where(low_rows, 1.0, 0.0)
    half_masks = [one_low.astype(BF), (1.0 - one_low).astype(BF)]

    loads[0].wait()
    loads[1].wait()

    for p in range(4):
        position = seq * TOKENS + lax.broadcasted_iota(jnp.int32, (TOKENS, 128), 0)
        scale = lax.rsqrt((position.astype(F32) + 1.0) * HEAD_WIDTH)
        folded = []
        for g in range(2):
            total = None
            for j in range(2):
                col = span(p * 512 + g * 256 + j * 128, 128)
                tile = (r.o[:, col].astype(F32) * scale).astype(BF)
                r.s[:, col] = tile
                m = dot(r.q[:, col], tile, ((0,), (0,)))
                total = m if total is None else total + m
            both = jnp.where(low64, total[:64], total[64:])
            folded.append(both + pltpu.roll(both, 64, 1))
        r.st_s[0, p] = jnp.where(low64, folded[0], folded[1])

    loads[2].wait()
    pl.semaphore_wait(barrier, len(peers))

    row_sum, row_sums = (r.st_t0, r.st_t1), (r.st_r20, r.st_r21)

    def state_first(i):
        for d in FAR_FIRST_4:
            xp = turned(x, d, 4)
            send(r.st_s.at[i, xp], r.st_r1.at[i, x], r.st_ss.at[i, 0], r.st_rs.at[i, 0], x=xp)
        r.st_r1[i, x] = r.st_s[i, x]

    def state_second(i):
        take_bytes(r.st_r1.at[i, pl.ds(0, 3)], r.st_rs.at[i, 0])
        total = sum(r.st_r1[i, p] for p in range(4)).astype(row_sum[i].dtype)
        row_sum[i][...] = total
        for d in range(1, 4):
            zp = turned(zl, d, 4)
            send(row_sum[i], row_sums[i].at[zl], r.st_ss.at[i, 1], r.st_rs.at[i, 1], zl=zp)
        row_sums[i][zl] = total

    def state_third(i):
        take_bytes(row_sums[i].at[pl.ds(0, 3)], r.st_rs.at[i, 1])
        rows = jnp.zeros((64, 128), F32)
        for z in range(4):
            counts = z > zl if i == 0 else z < zl
            rows = rows + jnp.where(counts, row_sums[i][z].astype(F32), 0.0)
        for xp in range(4):
            value = rows
            for p in range(xp + 1, 4) if i == 0 else range(xp):
                value = value + r.st_r1[i, p]
            r.st_o[i, xp] = value.astype(BF)
        for d in FAR_FIRST_4:
            xp = turned(x, d, 4)
            send(r.st_o.at[i, xp], r.st_r3.at[i, x], r.st_ss.at[i, 2], r.st_rs.at[i, 2], x=xp)
        r.st_r3[i, x] = r.st_o[i, x]

    def state_wait(i):
        take_bytes(r.st_r3.at[i, pl.ds(0, 3)], r.st_rs.at[i, 2])

    state_first(0)

    def shard_at(j, y_from, h):
        row = zh if j == 0 else 1 - zh
        return r.wb.at[row * 16 + y_from * 2 + c, pl.ds(h * 32, 32)]

    def to_partner(j, piece):
        send(piece, piece, r.wd_s.at[0], r.wd_r.at[j], c=1 - c)

    def along(way, j, step, h, piece, hops=1):
        yp = turned(y, hops if way == 0 else 8 - hops, 8)
        send(piece, piece, r.wr_s.at[0], r.wr_r.at[way, j, step - 1 + 4 * h], y=yp)

    def begin(j, h):
        piece = shard_at(j, y, h)
        along(0, j, 1, h, piece)
        along(1, j, 1, h, piece)
        to_partner(j, piece)

    def relay(step, j, ways=(0, 1)):
        for h in range(2):
            for way in ways:
                piece = shard_at(j, turned(y, 8 - step if way == 0 else step, 8), h)
                take_bytes(piece, r.wr_r.at[way, j, step - 1 + 4 * h])
                if step == 2 and way == j:
                    along(way, j, 4, h, piece, 2)
                if step < 3:
                    along(way, j, step + 1, h, piece)
                to_partner(j, piece)

    for edge, targets in ((3, (1, 0)), (0, (2, 3))):

        @pl.when(zl == edge)
        def _():
            for h in range(2):
                piece = shard_at(0, y, h)
                for target in targets:
                    send(piece, piece, r.wz_s.at[0], r.wz_r.at[h], zh=1 - zh, zl=target)

    begin(0, 0)
    begin(0, 1)
    loads[4].wait()
    send(r.x, r.x2, r.xx_s.at[0], r.xx_r.at[0], c=1 - c)

    loads[3].wait()
    t_row = lax.broadcasted_iota(jnp.int32, (TOKENS, TOKENS), 0)
    t_col = lax.broadcasted_iota(jnp.int32, (TOKENS, TOKENS), 1)

    def doubled(pair, g):
        pair = pair.astype(F32)
        other = pltpu.roll(pair, 64, 1)
        low, high = (pair, other) if g == 0 else (other, pair)
        return jnp.where(low_rows, low, high).astype(BF)

    def folded_pair(totals):
        ends = [t + pltpu.roll(t, 64, 1) for t in totals]
        return jnp.where(low_rows, ends[0], ends[1])

    def key_scores(p):
        pair_col = span(p * 128, 128)
        r.kt[pair_col, :] = r.k[:, pair_col].T
        totals = []
        for g in range(2):
            twice = doubled(r.k[:, pair_col], g)
            total = None
            for j in range(2):
                col = span(p * 512 + g * 256 + j * 128, 128)
                q_tile, s_tile = r.q[:, col], r.s[:, col]
                for half in half_masks:
                    scores = dot(twice, q_tile * half, ((1,), (1,)))
                    scores = jnp.where(t_col >= t_row, scores, 0.0).astype(BF)
                    part = dot(scores, s_tile * half)
                    total = part if total is None else total + part
            totals.append(total)
        r.vgi[:, pair_col] = folded_pair(totals)

    def transpose(src, dst, first, last):
        for n in range(first, last):
            rows = span(n * 128, 128)
            dst[rows, :] = src[:, rows].T

    for p in range(3):
        key_scores(p)
    state_second(0)
    relay(1, 0)
    key_scores(3)
    for h in range(2):
        take_bytes(shard_at(1, y, h), r.wz_r.at[h])
        begin(1, h)
    transpose(r.x, r.xt, 0, 16)
    relay(2, 0)
    take_bytes(r.x2, r.xx_r.at[0])
    transpose(r.x2, r.x2t, 0, 16)
    state_third(0)
    relay(1, 1)
    state_wait(0)

    for p in range(4):
        pair = r.st_r3[0, p].astype(F32)
        block = jnp.concatenate(
            [jnp.where(low64, pair, 0.0), jnp.where(low64, 0.0, pair)], axis=0
        ).astype(BF)
        r.bd[p] = block
        cols = slice(p * 128, p * 128 + 128)
        total = r.vgi[:, cols] + dot(r.k[:, cols], block)
        r.vg[p // 2, :, (p % 2) * 128 : (p % 2) * 128 + 128] = total.astype(BF)
    send(r.vg.at[1 - c], r.vgp, r.vv_s.at[0], r.vv_r.at[0], c=1 - c)
    relay(3, 0)
    relay(2, 1)
    take_bytes(r.vgp, r.vv_r.at[0])

    vg_own = r.vg[c]
    vg_other = r.vgp[...]
    for zp in range(2):
        for yp in range(8):
            rows = span(zp * 1024 + yp * 128, 128)
            part = (dot(r.xt[rows, :], vg_own) + dot(r.x2t[rows, :], vg_other)).astype(BF)
            for u in range(4):
                r.ga[u, yp, zp] = part[16 * u : 16 * u + 16]
                r.gb[yp, zp, u] = part[64 + 16 * u : 80 + 16 * u, :128]
                r.gc[zp, u, yp] = part[64 + 16 * u : 80 + 16 * u, 128:]

    z = zh * 4 + zl

    def z_at(d):
        place = turned(z, d, 8)
        return lax.div(place, 4), lax.rem(place, 4)

    for d in FAR_FIRST_4:
        xp = turned(x, d, 4)
        send(r.ga.at[xp], r.a1.at[d - 1], r.rs_s.at[0, 0], r.rs_r.at[0, 0], x=xp)
    for d in FAR_FIRST_8:
        hp, lp = z_at(d)
        send(r.gc.at[hp, lp], r.c1.at[d - 1], r.rs_s.at[2, 0], r.rs_r.at[2, 0], zh=hp, zl=lp)

    for d in FAR_FIRST_8:
        yp = turned(y, d, 8)
        send(r.gb.at[yp], r.b1.at[d - 1], r.rs_s.at[1, 0], r.rs_r.at[1, 0], y=yp)
    relay(4, 0, (0,))
    relay(3, 1)
    relay(4, 1, (1,))

    take_bytes(r.a1, r.rs_r.at[0, 0])

    for yp in range(8):
        total = r.ga[x, yp].astype(F32)
        for d in range(3):
            total = total + r.a1[d, yp].astype(F32)
        r.a2s[yp] = total.astype(BF)

    for d in FAR_FIRST_8:
        yp = turned(y, d, 8)
        send(r.a2s.at[yp], r.a2r.at[d - 1], r.rs_s.at[0, 1], r.rs_r.at[0, 1], y=yp)

    take_bytes(r.wb.at[pl.ds(0, 8)], r.wd_r.at[0])
    take_bytes(r.wb.at[pl.ds(0, 8)], r.wd_r.at[1])
    whole = r.wb[...].reshape(WIDTH, KV_WIDTH)
    r.v[...] = dot(r.x[...], whole).astype(BF)
    for p in range(4):
        cols = slice(p * 128, p * 128 + 128)
        m = dot(r.v[:, cols], r.k[:, cols], ((0,), (0,)))
        r.st_s[1, p] = jnp.where(low64, m[:64], m[64:])
    state_first(1)

    def value_scores(p):
        pair_col = span(p * 128, 128)
        totals = []
        for g in range(2):
            v_twice = doubled(r.v[:, pair_col], g)
            k_rows = r.kt[p * 128 + g * 64 : p * 128 + g * 64 + 64, :]
            total = None
            for j in range(2):
                col = span(p * 512 + g * 256 + j * 128, 128)
                q_tile, s_tile = r.q[:, col], r.s[:, col]
                grads = []
                for half in half_masks:
                    scores = dot(v_twice, s_tile * half, ((1,), (1,)))
                    scores = jnp.where(t_col >= t_row, scores, 0.0).astype(BF)
                    grads.append(dot(k_rows, scores))
                    part = dot(scores, q_tile * half)
                    total = part if total is None else total + part
                r.qgi[:, col] = jnp.concatenate(grads, axis=0).T
            totals.append(total)
        total = folded_pair(totals) + dot(r.v[:, pair_col], r.bd[p], ((1,), (1,)))
        r.kgo[:, pair_col] = total.astype(BF)

    value_scores(0)
    take_bytes(r.b1, r.rs_r.at[1, 0])
    for zp in range(2):
        for u in range(4):
            total = r.gb[y, zp, u].astype(F32)
            for d in range(7):
                total = total + r.b1[d, zp, u].astype(F32)
            r.b2s[u, zp] = total.astype(BF)
    for d in FAR_FIRST_4:
        xp = turned(x, d, 4)
        send(r.b2s.at[xp], r.b2r.at[d - 1], r.rs_s.at[1, 1], r.rs_r.at[1, 1], x=xp)

    take_bytes(r.c1, r.rs_r.at[2, 0])
    for yp in range(8):
        total = r.gc[zh, zl, yp].astype(F32)
        for d in range(7):
            total = total + r.c1[d, yp].astype(F32)
        r.c2s[yp] = total.astype(BF)
    for d in FAR_FIRST_8:
        yp = turned(y, d, 8)
        send(r.c2s.at[yp], r.c2r.at[d - 1], r.rs_s.at[2, 1], r.rs_r.at[2, 1], y=yp)

    value_scores(1)
    value_scores(2)
    state_second(1)

    take_bytes(r.a2r, r.rs_r.at[0, 1])
    for zp in range(2):
        total = r.a2s[y, zp].astype(F32)
        for d in range(7):
            total = total + r.a2r[d, zp].astype(F32)
        r.a3s[zp] = total.astype(BF)
    for d in FAR_FIRST_8:
        hp, lp = z_at(d)
        send(r.a3s.at[hp], r.a3r.at[d - 1], r.rs_s.at[0, 2], r.rs_r.at[0, 2], zh=hp, zl=lp)

    take_bytes(r.b2r, r.rs_r.at[1, 1])
    for zp in range(2):
        total = r.b2s[x, zp].astype(F32)
        for d in range(3):
            total = total + r.b2r[d, zp].astype(F32)
        r.b3s[zp] = total.astype(BF)
    for d in FAR_FIRST_8:
        hp, lp = z_at(d)
        send(r.b3s.at[hp], r.b3r.at[d - 1], r.rs_s.at[1, 2], r.rs_r.at[1, 2], zh=hp, zl=lp)

    take_bytes(r.c2r, r.rs_r.at[2, 1])
    total = r.c2s[y].astype(F32)
    for d in range(7):
        total = total + r.c2r[d].astype(F32)
    r.c3s[...] = total.astype(BF)
    for d in FAR_FIRST_4:
        xp = turned(x, d, 4)
        send(r.c3s, r.c3r.at[d - 1], r.rs_s.at[2, 2], r.rs_r.at[2, 2], x=xp)

    value_scores(3)
    state_third(1)

    vg_whole = jnp.concatenate([r.vg[0], r.vg[1]], axis=1)

    for n in range(8):
        rows = r.wb[pl.ds(n * 4, 4)].reshape(256, KV_WIDTH)
        col = span(n * 256, 256)
        r.igo[:, col] = dot(vg_whole, rows, ((1,), (1,))).astype(BF)


    factor = 1.0 / math.sqrt(TOKEN_COUNT)
    here_x, here_zl = c * 4 + x, c * 4 + zl

    def spread(src, dst, part, axis, at):
        target = 0 if part == 0 else 1
        for d in FAR_FIRST_4:
            where = {axis: turned(at, d, 4), "c": target}
            send(src, dst, r.rs_s.at[part, 3], r.rs_r.at[part, 3], **where)

        @pl.when(c != target)
        def _():
            send(src, dst, r.rs_s.at[part, 3], r.rs_r.at[part, 3], c=target)

    take_bytes(r.a3r, r.rs_r.at[0, 2])
    total = r.a3s[zh].astype(F32)
    for d in range(7):
        total = total + r.a3r[d].astype(F32)
    r.fa[...] = total * factor
    spread(r.fa, r.wga.at[here_x], 0, "x", x)
    take_bytes(r.c3r, r.rs_r.at[2, 2])
    total = r.c3s[...].astype(F32)
    for d in range(3):
        total = total + r.c3r[d].astype(F32)
    r.fc[...] = total * factor
    spread(r.fc, r.wgc.at[here_zl], 2, "zl", zl)
    take_bytes(r.b3r, r.rs_r.at[1, 2])
    total = r.b3s[zh].astype(F32)
    for d in range(7):
        total = total + r.b3r[d].astype(F32)
    r.fb[...] = total * factor
    spread(r.fb, r.wgb.at[here_x], 1, "x", x)

    state_wait(1)

    for p in range(4):
        pair = r.st_r3[1, p].astype(F32)
        other_way = pltpu.roll(pair, 64, 1)
        for g in range(2):
            low, high = (pair, other_way) if g == 0 else (other_way, pair)
            block = jnp.concatenate(
                [jnp.where(low64, low, 0.0), jnp.where(low64, 0.0, high)], axis=0
            ).astype(BF)
            for j in range(2):
                col = span(p * 512 + g * 256 + j * 128, 128)
                r.qgo[:, col] = (r.qgi[:, col] + dot(r.s[:, col], block)).astype(BF)


    @pl.when(c == 0)
    def _():
        r.wga[here_x] = r.fa[...]
        take_bytes(r.wga.at[pl.ds(0, 7)], r.rs_r.at[0, 3])
        for n in range(8):
            cp, u = divmod(n, 4)
            r.wgo[16 * u : 16 * u + 16, 256 * cp : 256 * cp + 256] = r.wga[n]
        take_bytes(r.wga.at[pl.ds(0, 3)], r.rs_s.at[0, 3])
        take_bytes(r.wgb.at[pl.ds(0, 4)], r.rs_s.at[1, 3])
        take_bytes(r.wgc.at[pl.ds(0, 4)], r.rs_s.at[2, 3])

    @pl.when(c == 1)
    def _():
        r.wgb[here_x] = r.fb[...]
        r.wgc[here_zl] = r.fc[...]
        take_bytes(r.wgb.at[pl.ds(0, 7)], r.rs_r.at[1, 3])
        take_bytes(r.wgc.at[pl.ds(0, 7)], r.rs_r.at[2, 3])
        for n in range(8):
            cp, u = divmod(n, 4)
            r.wgo[16 * u : 16 * u + 16, 256 * cp : 256 * cp + 128] = r.wgb[n]
            r.wgo[16 * u : 16 * u + 16, 256 * cp + 128 : 256 * cp + 256] = r.wgc[n]
        take_bytes(r.wga.at[pl.ds(0, 4)], r.rs_s.at[0, 3])
        take_bytes(r.wgb.at[pl.ds(0, 3)], r.rs_s.at[1, 3])
        take_bytes(r.wgc.at[pl.ds(0, 3)], r.rs_s.at[2, 3])


    take_bytes(r.wb.at[pl.ds(0, 16)], r.wd_s.at[0])

    @pl.when((zl == 0) | (zl == 3))
    def _():
        take_bytes(r.wb.at[pl.ds(0, 2)], r.wz_s.at[0])

    take_bytes(r.wb.at[pl.ds(0, 14)], r.wr_s.at[0])
    take_bytes(r.x, r.xx_s.at[0])
    take_bytes(r.vgp, r.vv_s.at[0])
    for i in range(2):
        take_bytes(r.st_s.at[i, pl.ds(0, 3)], r.st_ss.at[i, 0])
        take_bytes(row_sums[i].at[pl.ds(0, 3)], r.st_ss.at[i, 1])
        take_bytes(r.st_o.at[i, pl.ds(0, 3)], r.st_ss.at[i, 2])
    sent = [
        [r.a1, r.a2r, r.a3r],
        [r.b1, r.b2r, r.b3r],
        [r.c1, r.c2r, r.c3r],
    ]
    for part in range(3):
        for n in range(3):
            take_bytes(sent[part][n], r.rs_s.at[part, n])


def put_out(*refs):
    copies = [
        pltpu.make_async_copy(refs[i], refs[i + 4], refs[8].at[i]) for i in range(4)
    ]
    for copy in copies:
        copy.start()
    for copy in copies:
        copy.wait()


def body(inputs, queries, keys, value_matrix, out_grad):
    anywhere = pl.BlockSpec(memory_space=pl.ANY)
    in_vmem = pl.BlockSpec(memory_space=pltpu.VMEM)
    results = pl.pallas_call(
        kernel,
        out_shape=tuple(jax.ShapeDtypeStruct(*spec) for spec in OUTS.values()),
        in_specs=[pl.BlockSpec(memory_space=pltpu.HBM)] * 5,
        out_specs=(in_vmem,) * 4,
        scratch_shapes=[pltpu.VMEM(*spec) for spec in VMEM_SCRATCH.values()]
        + [pltpu.SemaphoreType.DMA(shape) for shape in SEM_SCRATCH.values()],
        compiler_params=pltpu.CompilerParams(
            collective_id=0, has_side_effects=True, vmem_limit_bytes=40 << 20
        ),
    )(
        *(
            pltpu.with_memory_space_constraint(a, pltpu.HBM)
            for a in (inputs[0], queries[0], keys[0], value_matrix, out_grad[0])
        )
    )
    query_gradient, key_gradient, input_grad, weight_grad = pl.pallas_call(
        put_out,
        out_shape=tuple(jax.ShapeDtypeStruct(*spec) for spec in OUTS.values()),
        in_specs=[in_vmem] * 4,
        out_specs=(anywhere,) * 4,
        scratch_shapes=[pltpu.SemaphoreType.DMA((4,))],
        compiler_params=pltpu.CompilerParams(vmem_limit_bytes=8 << 20),
    )(*results)
    return query_gradient[None], key_gradient[None], input_grad[None], weight_grad


def solution(mesh):
    torus = Mesh(mesh.devices.reshape(4, 4, 2, 8, 2), AXES)
    wide = P(DP, SEQ, None)
    return jax.shard_map(
        body,
        mesh=torus,
        in_specs=(wide, wide, wide, P(DP, None), wide),
        out_specs=(wide, wide, wide, P(DP, None)),
        check_vma=False,
    )
```

```python
import math
from types import SimpleNamespace

import jax
import jax.numpy as jnp
from jax import lax
from jax.experimental import pallas as pl
from jax.experimental.pallas import tpu as pltpu
from jax.sharding import Mesh
from jax.sharding import PartitionSpec as P

TOKENS = 192
WIDTH = 2048
KV_WIDTH = 512
HEAD_WIDTH = 64
GROUPS = 8
SEQ = ("zl", "x")
DP = ("zh", "y", "c")
AXES = ("zl", "x", "zh", "y", "c")
BF = jnp.bfloat16
F32 = jnp.float32
MESH = pl.DeviceIdType.MESH
TOKEN_COUNT = 98304
FAR_FIRST_4 = (2, 1, 3)
FAR_FIRST_8 = (4, 3, 5, 2, 6, 1, 7)

OUTS = dict(
    qgo=((TOKENS, WIDTH), BF),
    kgo=((TOKENS, KV_WIDTH), BF),
    igo=((TOKENS, WIDTH), BF),
    wgo=((64, KV_WIDTH), F32),
)
VMEM_SCRATCH = dict(
    x=((TOKENS, WIDTH), BF),
    x2=((TOKENS, WIDTH), BF),
    q=((TOKENS, WIDTH), BF),
    o=((TOKENS, WIDTH), BF),
    s=((TOKENS, WIDTH), BF),
    k=((TOKENS, KV_WIDTH), BF),
    kt=((KV_WIDTH, TOKENS), BF),
    v=((TOKENS, KV_WIDTH), BF),
    vf=((TOKENS, KV_WIDTH), F32),
    wb=((32, 64, KV_WIDTH), BF),
    vgi=((TOKENS, KV_WIDTH), F32),
    vg=((2, TOKENS, 256), BF),
    vgp=((TOKENS, 256), BF),
    bd=((4, 128, 128), BF),
    qgi=((TOKENS, WIDTH), F32),
    xt=((WIDTH, TOKENS), BF),
    x2t=((WIDTH, TOKENS), BF),
    st_s=((2, 4, 64, 128), F32),
    st_r1=((2, 4, 64, 128), F32),
    st_t0=((64, 128), BF),
    st_t1=((64, 128), BF),
    st_r20=((4, 64, 128), BF),
    st_r21=((4, 64, 128), BF),
    st_o=((2, 4, 64, 128), BF),
    st_r3=((2, 4, 64, 128), BF),
    ga=((4, 8, 2, 16, 256), BF),
    a1=((3, 8, 2, 16, 256), BF),
    a2s=((8, 2, 16, 256), BF),
    a2r=((7, 2, 16, 256), BF),
    a3s=((2, 16, 256), BF),
    a3r=((7, 16, 256), BF),
    gb=((8, 2, 4, 16, 128), BF),
    b1=((7, 2, 4, 16, 128), BF),
    b2s=((4, 2, 16, 128), BF),
    b2r=((3, 2, 16, 128), BF),
    b3s=((2, 16, 128), BF),
    b3r=((7, 16, 128), BF),
    gc=((2, 4, 8, 16, 128), BF),
    c1=((7, 8, 16, 128), BF),
    c2s=((8, 16, 128), BF),
    c2r=((7, 16, 128), BF),
    c3s=((16, 128), BF),
    c3r=((3, 16, 128), BF),
    fa=((16, 256), F32),
    fb=((16, 128), F32),
    fc=((16, 128), F32),
    wga=((8, 16, 256), F32),
    wgb=((8, 16, 128), F32),
    wgc=((8, 16, 128), F32),
)
SEM_SCRATCH = dict(
    ld=(5,),
    wd_s=(1,),
    wd_r=(2,),
    wz_s=(1,),
    wz_r=(2,),
    wr_s=(1,),
    wr_r=(2, 2, 8),
    xx_s=(1,),
    xx_r=(1,),
    vv_s=(1,),
    vv_r=(1,),
    st_ss=(2, 3),
    st_rs=(2, 3),
    rs_s=(3, 4),
    rs_r=(3, 4),
)


def dot(a, b, dims=((1,), (0,))):
    return lax.dot_general(a, b, (dims, ((), ())), preferred_element_type=F32)


def span(start, size):
    if isinstance(start, int):
        return slice(start, start + size)
    return pl.ds(pl.multiple_of(start, 128), size)


def take_bytes(ref, sem):
    pltpu.make_async_copy(ref, ref, sem).wait()


def kernel(x_h, q_h, k_h, w_h, o_h, *rest):
    r = SimpleNamespace(**dict(zip([*OUTS, *VMEM_SCRATCH, *SEM_SCRATCH], rest)))
    zl, x, zh, y, c = (lax.axis_index(a) for a in AXES)
    seq = zl * 4 + x

    def turned(value, step, size):
        return lax.rem(value + step, size)

    def send(src, dst, ssem, rsem, **where):
        pltpu.make_async_remote_copy(
            src, dst, ssem, rsem, device_id=where, device_id_type=MESH
        ).start()

    loads = [
        pltpu.make_async_copy(a, b, r.ld.at[i])
        for i, (a, b) in enumerate(
            [
                (o_h, r.o),
                (q_h, r.q),
                (w_h, r.wb.at[zh * 16 + y * 2 + c]),
                (k_h, r.k),
                (x_h, r.x),
            ]
        )
    ]
    for load in loads:
        load.start()

    peers = [dict(c=1 - c)]
    for d in range(1, 4):
        peers += [dict(x=turned(x, d, 4)), dict(x=turned(x, d, 4), c=1 - c)]
        peers += [dict(zl=turned(zl, d, 4)), dict(zl=turned(zl, d, 4), c=1 - c)]
    peers += [dict(zh=1 - zh, zl=turned(zl, d, 4)) for d in range(4)]
    peers += [dict(y=turned(y, d, 8)) for d in range(1, 8)]
    barrier = pltpu.get_barrier_semaphore()
    for peer in peers:
        pl.semaphore_signal(barrier, inc=1, device_id=peer, device_id_type=MESH)

    low64 = lax.broadcasted_iota(jnp.int32, (64, 128), 1) < 64
    low_rows = lax.broadcasted_iota(jnp.int32, (TOKENS, 128), 1) < 64
    one_low = jnp.where(low_rows, 1.0, 0.0)
    half_masks = [one_low.astype(BF), (1.0 - one_low).astype(BF)]

    loads[0].wait()
    loads[1].wait()

    for p in range(4):
        position = seq * TOKENS + lax.broadcasted_iota(jnp.int32, (TOKENS, 128), 0)
        scale = lax.rsqrt((position.astype(F32) + 1.0) * HEAD_WIDTH)
        folded = []
        for g in range(2):
            total = None
            for j in range(2):
                col = span(p * 512 + g * 256 + j * 128, 128)
                tile = (r.o[:, col].astype(F32) * scale).astype(BF)
                r.s[:, col] = tile
                m = dot(r.q[:, col], tile, ((0,), (0,)))
                total = m if total is None else total + m
            both = jnp.where(low64, total[:64], total[64:])
            folded.append(both + pltpu.roll(both, 64, 1))
        r.st_s[0, p] = jnp.where(low64, folded[0], folded[1])

    loads[2].wait()
    pl.semaphore_wait(barrier, len(peers))

    row_sum, row_sums = (r.st_t0, r.st_t1), (r.st_r20, r.st_r21)

    def state_first(i):
        for d in FAR_FIRST_4:
            xp = turned(x, d, 4)
            send(r.st_s.at[i, xp], r.st_r1.at[i, x], r.st_ss.at[i, 0], r.st_rs.at[i, 0], x=xp)
        r.st_r1[i, x] = r.st_s[i, x]

    def state_second(i):
        take_bytes(r.st_r1.at[i, pl.ds(0, 3)], r.st_rs.at[i, 0])
        total = sum(r.st_r1[i, p] for p in range(4)).astype(row_sum[i].dtype)
        row_sum[i][...] = total
        for d in (1, 2, 3) if i == 0 else (3, 2, 1):
            zp = turned(zl, d, 4)
            send(row_sum[i], row_sums[i].at[zl], r.st_ss.at[i, 1], r.st_rs.at[i, 1], zl=zp)
        row_sums[i][zl] = total

    def state_third(i):
        take_bytes(row_sums[i].at[pl.ds(0, 3)], r.st_rs.at[i, 1])
        rows = jnp.zeros((64, 128), F32)
        for z in range(4):
            counts = z > zl if i == 0 else z < zl
            rows = rows + jnp.where(counts, row_sums[i][z].astype(F32), 0.0)
        for xp in range(4):
            value = rows
            for p in range(xp + 1, 4) if i == 0 else range(xp):
                value = value + r.st_r1[i, p]
            r.st_o[i, xp] = value.astype(BF)
        for d in FAR_FIRST_4:
            xp = turned(x, d, 4)
            send(r.st_o.at[i, xp], r.st_r3.at[i, x], r.st_ss.at[i, 2], r.st_rs.at[i, 2], x=xp)
        r.st_r3[i, x] = r.st_o[i, x]

    def state_wait(i):
        take_bytes(r.st_r3.at[i, pl.ds(0, 3)], r.st_rs.at[i, 2])

    state_first(0)

    def shard_at(j, y_from, h):
        row = zh if j == 0 else 1 - zh
        return r.wb.at[row * 16 + y_from * 2 + c, pl.ds(h * 32, 32)]

    def to_partner(j, piece):
        send(piece, piece, r.wd_s.at[0], r.wd_r.at[j], c=1 - c)

    def along(way, j, step, h, piece, hops=1):
        yp = turned(y, hops if way == 0 else 8 - hops, 8)
        send(piece, piece, r.wr_s.at[0], r.wr_r.at[way, j, step - 1 + 4 * h], y=yp)

    def begin(j, h):
        piece = shard_at(j, y, h)
        along(0, j, 1, h, piece)
        along(1, j, 1, h, piece)
        to_partner(j, piece)

    def relay(step, j, ways=(0, 1)):
        for h in range(2):
            for way in ways:
                piece = shard_at(j, turned(y, 8 - step if way == 0 else step, 8), h)
                take_bytes(piece, r.wr_r.at[way, j, step - 1 + 4 * h])
                if step == 2 and way == j:
                    along(way, j, 4, h, piece, 2)
                if step < 3:
                    along(way, j, step + 1, h, piece)
                to_partner(j, piece)

    for edge, targets in ((3, (1, 0)), (0, (2, 3))):

        @pl.when(zl == edge)
        def _():
            for h in range(2):
                piece = shard_at(0, y, h)
                for target in targets:
                    send(piece, piece, r.wz_s.at[0], r.wz_r.at[h], zh=1 - zh, zl=target)

    begin(0, 0)
    begin(0, 1)
    loads[4].wait()
    send(r.x, r.x2, r.xx_s.at[0], r.xx_r.at[0], c=1 - c)

    loads[3].wait()
    t_row = lax.broadcasted_iota(jnp.int32, (TOKENS, TOKENS), 0)
    t_col = lax.broadcasted_iota(jnp.int32, (TOKENS, TOKENS), 1)

    def doubled(pair, g):
        pair = pair.astype(F32)
        other = pltpu.roll(pair, 64, 1)
        low, high = (pair, other) if g == 0 else (other, pair)
        return jnp.where(low_rows, low, high).astype(BF)

    def folded_pair(totals):
        ends = [t + pltpu.roll(t, 64, 1) for t in totals]
        return jnp.where(low_rows, ends[0], ends[1])

    def key_scores(p):
        pair_col = span(p * 128, 128)
        r.kt[pair_col, :] = r.k[:, pair_col].T
        totals = []
        for g in range(2):
            twice = doubled(r.k[:, pair_col], g)
            total = None
            for j in range(2):
                col = span(p * 512 + g * 256 + j * 128, 128)
                q_tile, s_tile = r.q[:, col], r.s[:, col]
                for half in half_masks:
                    scores = dot(twice, q_tile * half, ((1,), (1,)))
                    scores = jnp.where(t_col >= t_row, scores, 0.0).astype(BF)
                    part = dot(scores, s_tile * half)
                    total = part if total is None else total + part
            totals.append(total)
        r.vgi[:, pair_col] = folded_pair(totals)

    def transpose(src, dst, first, last):
        for n in range(first, last):
            rows = span(n * 128, 128)
            dst[rows, :] = src[:, rows].T

    for p in range(3):
        key_scores(p)
    state_second(0)
    relay(1, 0)
    key_scores(3)
    for h in range(2):
        take_bytes(shard_at(1, y, h), r.wz_r.at[h])
        begin(1, h)
    transpose(r.x, r.xt, 0, 16)
    take_bytes(r.x2, r.xx_r.at[0])
    transpose(r.x2, r.x2t, 0, 16)
    state_third(0)
    relay(2, 0)
    relay(1, 1)
    state_wait(0)

    for p in range(4):
        pair = r.st_r3[0, p].astype(F32)
        block = jnp.concatenate(
            [jnp.where(low64, pair, 0.0), jnp.where(low64, 0.0, pair)], axis=0
        ).astype(BF)
        r.bd[p] = block
        cols = slice(p * 128, p * 128 + 128)
        total = r.vgi[:, cols] + dot(r.k[:, cols], block)
        r.vg[p // 2, :, (p % 2) * 128 : (p % 2) * 128 + 128] = total.astype(BF)
    send(r.vg.at[1 - c], r.vgp, r.vv_s.at[0], r.vv_r.at[0], c=1 - c)
    relay(3, 0)
    relay(2, 1)
    take_bytes(r.vgp, r.vv_r.at[0])

    vg_own = r.vg[c]
    vg_other = r.vgp[...]
    for zp in range(2):
        for yp in range(8):
            rows = span(zp * 1024 + yp * 128, 128)
            part = (dot(r.xt[rows, :], vg_own) + dot(r.x2t[rows, :], vg_other)).astype(BF)
            for u in range(4):
                r.ga[u, yp, zp] = part[16 * u : 16 * u + 16]
                r.gb[yp, zp, u] = part[64 + 16 * u : 80 + 16 * u, :128]
                r.gc[zp, u, yp] = part[64 + 16 * u : 80 + 16 * u, 128:]

    z = zh * 4 + zl

    def z_at(d):
        place = turned(z, d, 8)
        return lax.div(place, 4), lax.rem(place, 4)

    for d in FAR_FIRST_4:
        xp = turned(x, d, 4)
        send(r.ga.at[xp], r.a1.at[d - 1], r.rs_s.at[0, 0], r.rs_r.at[0, 0], x=xp)
    for d in FAR_FIRST_8:
        hp, lp = z_at(d)
        send(r.gc.at[hp, lp], r.c1.at[d - 1], r.rs_s.at[2, 0], r.rs_r.at[2, 0], zh=hp, zl=lp)

    for d in FAR_FIRST_8:
        yp = turned(y, d, 8)
        send(r.gb.at[yp], r.b1.at[d - 1], r.rs_s.at[1, 0], r.rs_r.at[1, 0], y=yp)
    relay(4, 0, (0,))
    relay(3, 1)
    relay(4, 1, (1,))

    def values_part(row):
        half = r.wb[pl.ds(row * 16, 16)].reshape(WIDTH // 2, KV_WIDTH)
        return dot(r.x[:, span(row * 1024, 1024)], half)

    take_bytes(r.wb.at[pl.ds(0, 8)], r.wd_r.at[0])
    r.vf[...] = values_part(zh)

    take_bytes(r.a1, r.rs_r.at[0, 0])

    for yp in range(8):
        total = r.ga[x, yp].astype(F32)
        for d in range(3):
            total = total + r.a1[d, yp].astype(F32)
        r.a2s[yp] = total.astype(BF)

    for d in FAR_FIRST_8:
        yp = turned(y, d, 8)
        send(r.a2s.at[yp], r.a2r.at[d - 1], r.rs_s.at[0, 1], r.rs_r.at[0, 1], y=yp)

    take_bytes(r.wb.at[pl.ds(0, 8)], r.wd_r.at[1])
    r.v[...] = (r.vf[...] + values_part(1 - zh)).astype(BF)
    for p in range(4):
        cols = slice(p * 128, p * 128 + 128)
        m = dot(r.v[:, cols], r.k[:, cols], ((0,), (0,)))
        r.st_s[1, p] = jnp.where(low64, m[:64], m[64:])
    state_first(1)

    def value_scores(p):
        pair_col = span(p * 128, 128)
        totals = []
        for g in range(2):
            v_twice = doubled(r.v[:, pair_col], g)
            k_rows = r.kt[p * 128 + g * 64 : p * 128 + g * 64 + 64, :]
            total = None
            for j in range(2):
                col = span(p * 512 + g * 256 + j * 128, 128)
                q_tile, s_tile = r.q[:, col], r.s[:, col]
                grads = []
                for half in half_masks:
                    scores = dot(v_twice, s_tile * half, ((1,), (1,)))
                    scores = jnp.where(t_col >= t_row, scores, 0.0).astype(BF)
                    grads.append(dot(k_rows, scores))
                    part = dot(scores, q_tile * half)
                    total = part if total is None else total + part
                r.qgi[:, col] = jnp.concatenate(grads, axis=0).T
            totals.append(total)
        total = folded_pair(totals) + dot(r.v[:, pair_col], r.bd[p], ((1,), (1,)))
        r.kgo[:, pair_col] = total.astype(BF)

    value_scores(0)
    take_bytes(r.b1, r.rs_r.at[1, 0])
    for zp in range(2):
        for u in range(4):
            total = r.gb[y, zp, u].astype(F32)
            for d in range(7):
                total = total + r.b1[d, zp, u].astype(F32)
            r.b2s[u, zp] = total.astype(BF)
    for d in FAR_FIRST_4:
        xp = turned(x, d, 4)
        send(r.b2s.at[xp], r.b2r.at[d - 1], r.rs_s.at[1, 1], r.rs_r.at[1, 1], x=xp)

    take_bytes(r.c1, r.rs_r.at[2, 0])
    for yp in range(8):
        total = r.gc[zh, zl, yp].astype(F32)
        for d in range(7):
            total = total + r.c1[d, yp].astype(F32)
        r.c2s[yp] = total.astype(BF)
    for d in FAR_FIRST_8:
        yp = turned(y, d, 8)
        send(r.c2s.at[yp], r.c2r.at[d - 1], r.rs_s.at[2, 1], r.rs_r.at[2, 1], y=yp)

    value_scores(1)
    value_scores(2)
    state_second(1)

    take_bytes(r.a2r, r.rs_r.at[0, 1])
    for zp in range(2):
        total = r.a2s[y, zp].astype(F32)
        for d in range(7):
            total = total + r.a2r[d, zp].astype(F32)
        r.a3s[zp] = total.astype(BF)
    for d in FAR_FIRST_8:
        hp, lp = z_at(d)
        send(r.a3s.at[hp], r.a3r.at[d - 1], r.rs_s.at[0, 2], r.rs_r.at[0, 2], zh=hp, zl=lp)

    take_bytes(r.b2r, r.rs_r.at[1, 1])
    for zp in range(2):
        total = r.b2s[x, zp].astype(F32)
        for d in range(3):
            total = total + r.b2r[d, zp].astype(F32)
        r.b3s[zp] = total.astype(BF)
    for d in FAR_FIRST_8:
        hp, lp = z_at(d)
        send(r.b3s.at[hp], r.b3r.at[d - 1], r.rs_s.at[1, 2], r.rs_r.at[1, 2], zh=hp, zl=lp)

    take_bytes(r.c2r, r.rs_r.at[2, 1])
    total = r.c2s[y].astype(F32)
    for d in range(7):
        total = total + r.c2r[d].astype(F32)
    r.c3s[...] = total.astype(BF)
    for d in FAR_FIRST_4:
        xp = turned(x, d, 4)
        send(r.c3s, r.c3r.at[d - 1], r.rs_s.at[2, 2], r.rs_r.at[2, 2], x=xp)

    value_scores(3)
    state_third(1)

    vg_whole = jnp.concatenate([r.vg[0], r.vg[1]], axis=1)

    for n in range(8):
        rows = r.wb[pl.ds(n * 4, 4)].reshape(256, KV_WIDTH)
        col = span(n * 256, 256)
        r.igo[:, col] = dot(vg_whole, rows, ((1,), (1,))).astype(BF)


    factor = 1.0 / math.sqrt(TOKEN_COUNT)
    here_x, here_zl = c * 4 + x, c * 4 + zl

    def spread(src, dst, part, axis, at):
        target = 0 if part == 0 else 1
        for d in FAR_FIRST_4:
            where = {axis: turned(at, d, 4), "c": target}
            send(src, dst, r.rs_s.at[part, 3], r.rs_r.at[part, 3], **where)

        @pl.when(c != target)
        def _():
            send(src, dst, r.rs_s.at[part, 3], r.rs_r.at[part, 3], c=target)

    take_bytes(r.a3r, r.rs_r.at[0, 2])
    total = r.a3s[zh].astype(F32)
    for d in range(7):
        total = total + r.a3r[d].astype(F32)
    r.fa[...] = total * factor
    spread(r.fa, r.wga.at[here_x], 0, "x", x)
    take_bytes(r.c3r, r.rs_r.at[2, 2])
    total = r.c3s[...].astype(F32)
    for d in range(3):
        total = total + r.c3r[d].astype(F32)
    r.fc[...] = total * factor
    spread(r.fc, r.wgc.at[here_zl], 2, "zl", zl)
    take_bytes(r.b3r, r.rs_r.at[1, 2])
    total = r.b3s[zh].astype(F32)
    for d in range(7):
        total = total + r.b3r[d].astype(F32)
    r.fb[...] = total * factor
    spread(r.fb, r.wgb.at[here_x], 1, "x", x)

    state_wait(1)

    for p in range(4):
        pair = r.st_r3[1, p].astype(F32)
        other_way = pltpu.roll(pair, 64, 1)
        for g in range(2):
            low, high = (pair, other_way) if g == 0 else (other_way, pair)
            block = jnp.concatenate(
                [jnp.where(low64, low, 0.0), jnp.where(low64, 0.0, high)], axis=0
            ).astype(BF)
            for j in range(2):
                col = span(p * 512 + g * 256 + j * 128, 128)
                r.qgo[:, col] = (r.qgi[:, col] + dot(r.s[:, col], block)).astype(BF)


    @pl.when(c == 0)
    def _():
        r.wga[here_x] = r.fa[...]
        take_bytes(r.wga.at[pl.ds(0, 7)], r.rs_r.at[0, 3])
        for n in range(8):
            cp, u = divmod(n, 4)
            r.wgo[16 * u : 16 * u + 16, 256 * cp : 256 * cp + 256] = r.wga[n]
        take_bytes(r.wga.at[pl.ds(0, 3)], r.rs_s.at[0, 3])
        take_bytes(r.wgb.at[pl.ds(0, 4)], r.rs_s.at[1, 3])
        take_bytes(r.wgc.at[pl.ds(0, 4)], r.rs_s.at[2, 3])

    @pl.when(c == 1)
    def _():
        r.wgb[here_x] = r.fb[...]
        r.wgc[here_zl] = r.fc[...]
        take_bytes(r.wgb.at[pl.ds(0, 7)], r.rs_r.at[1, 3])
        take_bytes(r.wgc.at[pl.ds(0, 7)], r.rs_r.at[2, 3])
        for n in range(8):
            cp, u = divmod(n, 4)
            r.wgo[16 * u : 16 * u + 16, 256 * cp : 256 * cp + 128] = r.wgb[n]
            r.wgo[16 * u : 16 * u + 16, 256 * cp + 128 : 256 * cp + 256] = r.wgc[n]
        take_bytes(r.wga.at[pl.ds(0, 4)], r.rs_s.at[0, 3])
        take_bytes(r.wgb.at[pl.ds(0, 3)], r.rs_s.at[1, 3])
        take_bytes(r.wgc.at[pl.ds(0, 3)], r.rs_s.at[2, 3])


    take_bytes(r.wb.at[pl.ds(0, 16)], r.wd_s.at[0])

    @pl.when((zl == 0) | (zl == 3))
    def _():
        take_bytes(r.wb.at[pl.ds(0, 2)], r.wz_s.at[0])

    take_bytes(r.wb.at[pl.ds(0, 14)], r.wr_s.at[0])
    take_bytes(r.x, r.xx_s.at[0])
    take_bytes(r.vgp, r.vv_s.at[0])
    for i in range(2):
        take_bytes(r.st_s.at[i, pl.ds(0, 3)], r.st_ss.at[i, 0])
        take_bytes(row_sums[i].at[pl.ds(0, 3)], r.st_ss.at[i, 1])
        take_bytes(r.st_o.at[i, pl.ds(0, 3)], r.st_ss.at[i, 2])
    sent = [
        [r.a1, r.a2r, r.a3r],
        [r.b1, r.b2r, r.b3r],
        [r.c1, r.c2r, r.c3r],
    ]
    for part in range(3):
        for n in range(3):
            take_bytes(sent[part][n], r.rs_s.at[part, n])


def put_out(*refs):
    copies = [
        pltpu.make_async_copy(refs[i], refs[i + 4], refs[8].at[i]) for i in range(4)
    ]
    for copy in copies:
        copy.start()
    for copy in copies:
        copy.wait()


def body(inputs, queries, keys, value_matrix, out_grad):
    anywhere = pl.BlockSpec(memory_space=pl.ANY)
    in_vmem = pl.BlockSpec(memory_space=pltpu.VMEM)
    results = pl.pallas_call(
        kernel,
        out_shape=tuple(jax.ShapeDtypeStruct(*spec) for spec in OUTS.values()),
        in_specs=[pl.BlockSpec(memory_space=pltpu.HBM)] * 5,
        out_specs=(in_vmem,) * 4,
        scratch_shapes=[pltpu.VMEM(*spec) for spec in VMEM_SCRATCH.values()]
        + [pltpu.SemaphoreType.DMA(shape) for shape in SEM_SCRATCH.values()],
        compiler_params=pltpu.CompilerParams(
            collective_id=0, has_side_effects=True, vmem_limit_bytes=40 << 20
        ),
    )(
        *(
            pltpu.with_memory_space_constraint(a, pltpu.HBM)
            for a in (inputs[0], queries[0], keys[0], value_matrix, out_grad[0])
        )
    )
    query_gradient, key_gradient, input_grad, weight_grad = pl.pallas_call(
        put_out,
        out_shape=tuple(jax.ShapeDtypeStruct(*spec) for spec in OUTS.values()),
        in_specs=[in_vmem] * 4,
        out_specs=(anywhere,) * 4,
        scratch_shapes=[pltpu.SemaphoreType.DMA((4,))],
        compiler_params=pltpu.CompilerParams(vmem_limit_bytes=8 << 20),
    )(*results)
    return query_gradient[None], key_gradient[None], input_grad[None], weight_grad


def solution(mesh):
    torus = Mesh(mesh.devices.reshape(4, 4, 2, 8, 2), AXES)
    wide = P(DP, SEQ, None)
    return jax.shard_map(
        body,
        mesh=torus,
        in_specs=(wide, wide, wide, P(DP, None), wide),
        out_specs=(wide, wide, wide, P(DP, None)),
        check_vma=False,
    )
```

```python
import math
from types import SimpleNamespace

import jax
import jax.numpy as jnp
from jax import lax
from jax.experimental import pallas as pl
from jax.experimental.pallas import tpu as pltpu
from jax.sharding import Mesh
from jax.sharding import PartitionSpec as P

TOKENS = 192
WIDTH = 2048
KV_WIDTH = 512
HEAD_WIDTH = 64
GROUPS = 8
SEQ = ("zl", "x")
DP = ("zh", "y", "c")
AXES = ("zl", "x", "zh", "y", "c")
BF = jnp.bfloat16
F32 = jnp.float32
MESH = pl.DeviceIdType.MESH
TOKEN_COUNT = 98304
FAR_FIRST_4 = (2, 1, 3)
FAR_FIRST_8 = (4, 3, 5, 2, 6, 1, 7)

OUTS = dict(
    qgo=((TOKENS, WIDTH), BF),
    kgo=((TOKENS, KV_WIDTH), BF),
    igo=((TOKENS, WIDTH), BF),
    wgo=((64, KV_WIDTH), F32),
)
VMEM_SCRATCH = dict(
    x=((TOKENS, WIDTH), BF),
    x2=((TOKENS, WIDTH), BF),
    q=((TOKENS, WIDTH), BF),
    o=((TOKENS, WIDTH), BF),
    s=((TOKENS, WIDTH), BF),
    k=((TOKENS, KV_WIDTH), BF),
    kt=((KV_WIDTH, TOKENS), BF),
    v=((TOKENS, KV_WIDTH), BF),
    vf=((TOKENS, KV_WIDTH), F32),
    wb=((32, 64, KV_WIDTH), BF),
    vgi=((TOKENS, KV_WIDTH), F32),
    vg=((2, TOKENS, 256), BF),
    vgp=((TOKENS, 256), BF),
    bd=((4, 128, 128), BF),
    qgi=((TOKENS, WIDTH), F32),
    xt=((WIDTH, TOKENS), BF),
    x2t=((WIDTH, TOKENS), BF),
    st_s=((2, 4, 64, 128), F32),
    st_r1=((2, 4, 64, 128), F32),
    st_t0=((64, 128), BF),
    st_t1=((64, 128), BF),
    st_r20=((4, 64, 128), BF),
    st_r21=((4, 64, 128), BF),
    st_o=((2, 4, 64, 128), BF),
    st_r3=((2, 4, 64, 128), BF),
    ga=((4, 8, 2, 16, 256), BF),
    a1=((3, 8, 2, 16, 256), BF),
    a2s=((8, 2, 16, 256), BF),
    a2r=((7, 2, 16, 256), BF),
    a3s=((2, 16, 256), BF),
    a3r=((7, 16, 256), BF),
    gb=((8, 2, 4, 16, 128), BF),
    b1=((7, 2, 4, 16, 128), BF),
    b2s=((4, 2, 16, 128), BF),
    b2r=((3, 2, 16, 128), BF),
    b3s=((2, 16, 128), BF),
    b3r=((7, 16, 128), BF),
    gc=((2, 4, 8, 16, 128), BF),
    c1=((7, 8, 16, 128), BF),
    c2s=((8, 16, 128), BF),
    c2r=((7, 16, 128), BF),
    c3s=((16, 128), BF),
    c3r=((3, 16, 128), BF),
    fa=((16, 256), F32),
    fb=((16, 128), F32),
    fc=((16, 128), F32),
    wga=((8, 16, 256), F32),
    wgb=((8, 16, 128), F32),
    wgc=((8, 16, 128), F32),
)
SEM_SCRATCH = dict(
    ld=(5,),
    wd_s=(1,),
    wd_r=(2,),
    wz_s=(1,),
    wz_r=(2,),
    wr_s=(1,),
    wr_r=(2, 2, 8),
    xx_s=(1,),
    xx_r=(1,),
    vv_s=(1,),
    vv_r=(1,),
    st_ss=(2, 3),
    st_rs=(2, 3),
    rs_s=(3, 4),
    rs_r=(3, 4),
)


def dot(a, b, dims=((1,), (0,))):
    return lax.dot_general(a, b, (dims, ((), ())), preferred_element_type=F32)


def span(start, size):
    if isinstance(start, int):
        return slice(start, start + size)
    return pl.ds(pl.multiple_of(start, 128), size)


def take_bytes(ref, sem):
    pltpu.make_async_copy(ref, ref, sem).wait()


def kernel(x_h, q_h, k_h, w_h, o_h, *rest):
    r = SimpleNamespace(**dict(zip([*OUTS, *VMEM_SCRATCH, *SEM_SCRATCH], rest)))
    zl, x, zh, y, c = (lax.axis_index(a) for a in AXES)
    seq = zl * 4 + x

    def turned(value, step, size):
        return lax.rem(value + step, size)

    def send(src, dst, ssem, rsem, **where):
        pltpu.make_async_remote_copy(
            src, dst, ssem, rsem, device_id=where, device_id_type=MESH
        ).start()

    loads = [
        pltpu.make_async_copy(a, b, r.ld.at[i])
        for i, (a, b) in enumerate(
            [
                (o_h, r.o),
                (q_h, r.q),
                (w_h, r.wb.at[zh * 16 + y * 2 + c]),
                (k_h, r.k),
                (x_h, r.x),
            ]
        )
    ]
    for load in loads:
        load.start()

    peers = [dict(c=1 - c)]
    for d in range(1, 4):
        peers += [dict(x=turned(x, d, 4)), dict(x=turned(x, d, 4), c=1 - c)]
        peers += [dict(zl=turned(zl, d, 4)), dict(zl=turned(zl, d, 4), c=1 - c)]
    peers += [dict(zh=1 - zh, zl=turned(zl, d, 4)) for d in range(4)]
    peers += [dict(y=turned(y, d, 8)) for d in range(1, 8)]
    barrier = pltpu.get_barrier_semaphore()
    for peer in peers:
        pl.semaphore_signal(barrier, inc=1, device_id=peer, device_id_type=MESH)

    low64 = lax.broadcasted_iota(jnp.int32, (64, 128), 1) < 64
    low_rows = lax.broadcasted_iota(jnp.int32, (TOKENS, 128), 1) < 64
    one_low = jnp.where(low_rows, 1.0, 0.0)
    half_masks = [one_low.astype(BF), (1.0 - one_low).astype(BF)]

    loads[0].wait()
    loads[1].wait()

    for p in range(4):
        position = seq * TOKENS + lax.broadcasted_iota(jnp.int32, (TOKENS, 128), 0)
        scale = lax.rsqrt((position.astype(F32) + 1.0) * HEAD_WIDTH)
        folded = []
        for g in range(2):
            total = None
            for j in range(2):
                col = span(p * 512 + g * 256 + j * 128, 128)
                tile = (r.o[:, col].astype(F32) * scale).astype(BF)
                r.s[:, col] = tile
                m = dot(r.q[:, col], tile, ((0,), (0,)))
                total = m if total is None else total + m
            both = jnp.where(low64, total[:64], total[64:])
            folded.append(both + pltpu.roll(both, 64, 1))
        r.st_s[0, p] = jnp.where(low64, folded[0], folded[1])

    loads[2].wait()
    pl.semaphore_wait(barrier, len(peers))

    row_sum, row_sums = (r.st_t0, r.st_t1), (r.st_r20, r.st_r21)

    def state_first(i):
        for d in FAR_FIRST_4:
            xp = turned(x, d, 4)
            send(r.st_s.at[i, xp], r.st_r1.at[i, x], r.st_ss.at[i, 0], r.st_rs.at[i, 0], x=xp)
        r.st_r1[i, x] = r.st_s[i, x]

    def state_second(i):
        take_bytes(r.st_r1.at[i, pl.ds(0, 3)], r.st_rs.at[i, 0])
        total = sum(r.st_r1[i, p] for p in range(4)).astype(row_sum[i].dtype)
        row_sum[i][...] = total
        for d in range(1, 4):
            zp = turned(zl, d, 4)
            send(row_sum[i], row_sums[i].at[zl], r.st_ss.at[i, 1], r.st_rs.at[i, 1], zl=zp)
        row_sums[i][zl] = total

    def state_third(i):
        take_bytes(row_sums[i].at[pl.ds(0, 3)], r.st_rs.at[i, 1])
        rows = jnp.zeros((64, 128), F32)
        for z in range(4):
            counts = z > zl if i == 0 else z < zl
            rows = rows + jnp.where(counts, row_sums[i][z].astype(F32), 0.0)
        for xp in range(4):
            value = rows
            for p in range(xp + 1, 4) if i == 0 else range(xp):
                value = value + r.st_r1[i, p]
            r.st_o[i, xp] = value.astype(BF)
        for d in FAR_FIRST_4:
            xp = turned(x, d, 4)
            send(r.st_o.at[i, xp], r.st_r3.at[i, x], r.st_ss.at[i, 2], r.st_rs.at[i, 2], x=xp)
        r.st_r3[i, x] = r.st_o[i, x]

    def state_wait(i):
        take_bytes(r.st_r3.at[i, pl.ds(0, 3)], r.st_rs.at[i, 2])

    state_first(0)

    def shard_at(j, y_from, h):
        row = zh if j == 0 else 1 - zh
        return r.wb.at[row * 16 + y_from * 2 + c, pl.ds(h * 32, 32)]

    def to_partner(j, piece):
        send(piece, piece, r.wd_s.at[0], r.wd_r.at[j], c=1 - c)

    def along(way, j, step, h, piece, hops=1):
        yp = turned(y, hops if way == 0 else 8 - hops, 8)
        send(piece, piece, r.wr_s.at[0], r.wr_r.at[way, j, step - 1 + 4 * h], y=yp)

    def begin(j, h):
        piece = shard_at(j, y, h)
        along(0, j, 1, h, piece)
        along(1, j, 1, h, piece)
        to_partner(j, piece)

    def relay(step, j, ways=(0, 1)):
        for h in range(2):
            for way in ways:
                piece = shard_at(j, turned(y, 8 - step if way == 0 else step, 8), h)
                take_bytes(piece, r.wr_r.at[way, j, step - 1 + 4 * h])
                if step == 2 and way == j:
                    along(way, j, 4, h, piece, 2)
                if step < 3:
                    along(way, j, step + 1, h, piece)
                to_partner(j, piece)

    for edge, targets in ((3, (1, 0)), (0, (2, 3))):

        @pl.when(zl == edge)
        def _():
            for h in range(2):
                piece = shard_at(0, y, h)
                for target in targets:
                    send(piece, piece, r.wz_s.at[0], r.wz_r.at[h], zh=1 - zh, zl=target)

    begin(0, 0)
    begin(0, 1)
    loads[4].wait()
    send(r.x, r.x2, r.xx_s.at[0], r.xx_r.at[0], c=1 - c)

    loads[3].wait()
    t_row = lax.broadcasted_iota(jnp.int32, (TOKENS, TOKENS), 0)
    t_col = lax.broadcasted_iota(jnp.int32, (TOKENS, TOKENS), 1)

    def doubled(pair, g):
        pair = pair.astype(F32)
        other = pltpu.roll(pair, 64, 1)
        low, high = (pair, other) if g == 0 else (other, pair)
        return jnp.where(low_rows, low, high).astype(BF)

    def folded_pair(totals):
        ends = [t + pltpu.roll(t, 64, 1) for t in totals]
        return jnp.where(low_rows, ends[0], ends[1])

    def key_scores(p):
        pair_col = span(p * 128, 128)
        r.kt[pair_col, :] = r.k[:, pair_col].T
        totals = []
        for g in range(2):
            twice = doubled(r.k[:, pair_col], g)
            total = None
            for j in range(2):
                col = span(p * 512 + g * 256 + j * 128, 128)
                q_tile, s_tile = r.q[:, col], r.s[:, col]
                for half in half_masks:
                    scores = dot(twice, q_tile * half, ((1,), (1,)))
                    scores = jnp.where(t_col >= t_row, scores, 0.0).astype(BF)
                    part = dot(scores, s_tile * half)
                    total = part if total is None else total + part
            totals.append(total)
        r.vgi[:, pair_col] = folded_pair(totals)

    def transpose(src, dst, first, last):
        for n in range(first, last):
            rows = span(n * 128, 128)
            dst[rows, :] = src[:, rows].T

    for p in range(3):
        key_scores(p)
    state_second(0)
    relay(1, 0)
    key_scores(3)
    for h in range(2):
        take_bytes(shard_at(1, y, h), r.wz_r.at[h])
        begin(1, h)
    transpose(r.x, r.xt, 0, 16)
    relay(2, 0)
    take_bytes(r.x2, r.xx_r.at[0])
    transpose(r.x2, r.x2t, 0, 16)
    state_third(0)
    relay(1, 1)
    state_wait(0)

    for p in range(4):
        pair = r.st_r3[0, p].astype(F32)
        block = jnp.concatenate(
            [jnp.where(low64, pair, 0.0), jnp.where(low64, 0.0, pair)], axis=0
        ).astype(BF)
        r.bd[p] = block
        cols = slice(p * 128, p * 128 + 128)
        total = r.vgi[:, cols] + dot(r.k[:, cols], block)
        r.vg[p // 2, :, (p % 2) * 128 : (p % 2) * 128 + 128] = total.astype(BF)
    send(r.vg.at[1 - c], r.vgp, r.vv_s.at[0], r.vv_r.at[0], c=1 - c)
    relay(3, 0)
    relay(2, 1)
    take_bytes(r.vgp, r.vv_r.at[0])

    vg_own = r.vg[c]
    vg_other = r.vgp[...]
    for zp in range(2):
        for yp in range(8):
            rows = span(zp * 1024 + yp * 128, 128)
            part = (dot(r.xt[rows, :], vg_own) + dot(r.x2t[rows, :], vg_other)).astype(BF)
            for u in range(4):
                r.ga[u, yp, zp] = part[16 * u : 16 * u + 16]
                r.gb[yp, zp, u] = part[64 + 16 * u : 80 + 16 * u, :128]
                r.gc[zp, u, yp] = part[64 + 16 * u : 80 + 16 * u, 128:]

    z = zh * 4 + zl

    def z_at(d):
        place = turned(z, d, 8)
        return lax.div(place, 4), lax.rem(place, 4)

    for d in FAR_FIRST_4:
        xp = turned(x, d, 4)
        send(r.ga.at[xp], r.a1.at[d - 1], r.rs_s.at[0, 0], r.rs_r.at[0, 0], x=xp)
    for d in FAR_FIRST_8:
        hp, lp = z_at(d)
        send(r.gc.at[hp, lp], r.c1.at[d - 1], r.rs_s.at[2, 0], r.rs_r.at[2, 0], zh=hp, zl=lp)

    for d in FAR_FIRST_8:
        yp = turned(y, d, 8)
        send(r.gb.at[yp], r.b1.at[d - 1], r.rs_s.at[1, 0], r.rs_r.at[1, 0], y=yp)
    relay(4, 0, (0,))
    relay(3, 1)
    relay(4, 1, (1,))

    def values_part(row):
        half = r.wb[pl.ds(row * 16, 16)].reshape(WIDTH // 2, KV_WIDTH)
        return dot(r.x[:, span(row * 1024, 1024)], half)

    take_bytes(r.wb.at[pl.ds(0, 8)], r.wd_r.at[0])
    r.vf[...] = values_part(zh)

    take_bytes(r.a1, r.rs_r.at[0, 0])

    for yp in range(8):
        total = r.ga[x, yp].astype(F32)
        for d in range(3):
            total = total + r.a1[d, yp].astype(F32)
        r.a2s[yp] = total.astype(BF)

    for d in FAR_FIRST_8:
        yp = turned(y, d, 8)
        send(r.a2s.at[yp], r.a2r.at[d - 1], r.rs_s.at[0, 1], r.rs_r.at[0, 1], y=yp)

    take_bytes(r.wb.at[pl.ds(0, 8)], r.wd_r.at[1])
    r.v[...] = (r.vf[...] + values_part(1 - zh)).astype(BF)
    for p in range(4):
        cols = slice(p * 128, p * 128 + 128)
        m = dot(r.v[:, cols], r.k[:, cols], ((0,), (0,)))
        r.st_s[1, p] = jnp.where(low64, m[:64], m[64:])
    state_first(1)

    def value_scores(p):
        pair_col = span(p * 128, 128)
        totals = []
        for g in range(2):
            v_twice = doubled(r.v[:, pair_col], g)
            k_rows = r.kt[p * 128 + g * 64 : p * 128 + g * 64 + 64, :]
            total = None
            for j in range(2):
                col = span(p * 512 + g * 256 + j * 128, 128)
                q_tile, s_tile = r.q[:, col], r.s[:, col]
                grads = []
                for half in half_masks:
                    scores = dot(v_twice, s_tile * half, ((1,), (1,)))
                    scores = jnp.where(t_col >= t_row, scores, 0.0).astype(BF)
                    grads.append(dot(k_rows, scores))
                    part = dot(scores, q_tile * half)
                    total = part if total is None else total + part
                r.qgi[:, col] = jnp.concatenate(grads, axis=0).T
            totals.append(total)
        total = folded_pair(totals) + dot(r.v[:, pair_col], r.bd[p], ((1,), (1,)))
        r.kgo[:, pair_col] = total.astype(BF)

    value_scores(0)
    take_bytes(r.b1, r.rs_r.at[1, 0])
    for zp in range(2):
        for u in range(4):
            total = r.gb[y, zp, u].astype(F32)
            for d in range(7):
                total = total + r.b1[d, zp, u].astype(F32)
            r.b2s[u, zp] = total.astype(BF)
    for d in FAR_FIRST_4:
        xp = turned(x, d, 4)
        send(r.b2s.at[xp], r.b2r.at[d - 1], r.rs_s.at[1, 1], r.rs_r.at[1, 1], x=xp)

    take_bytes(r.c1, r.rs_r.at[2, 0])
    for yp in range(8):
        total = r.gc[zh, zl, yp].astype(F32)
        for d in range(7):
            total = total + r.c1[d, yp].astype(F32)
        r.c2s[yp] = total.astype(BF)
    for d in FAR_FIRST_8:
        yp = turned(y, d, 8)
        send(r.c2s.at[yp], r.c2r.at[d - 1], r.rs_s.at[2, 1], r.rs_r.at[2, 1], y=yp)

    value_scores(1)
    value_scores(2)
    state_second(1)

    take_bytes(r.a2r, r.rs_r.at[0, 1])
    for zp in range(2):
        total = r.a2s[y, zp].astype(F32)
        for d in range(7):
            total = total + r.a2r[d, zp].astype(F32)
        r.a3s[zp] = total.astype(BF)
    for d in FAR_FIRST_8:
        hp, lp = z_at(d)
        send(r.a3s.at[hp], r.a3r.at[d - 1], r.rs_s.at[0, 2], r.rs_r.at[0, 2], zh=hp, zl=lp)

    take_bytes(r.b2r, r.rs_r.at[1, 1])
    for zp in range(2):
        total = r.b2s[x, zp].astype(F32)
        for d in range(3):
            total = total + r.b2r[d, zp].astype(F32)
        r.b3s[zp] = total.astype(BF)
    for d in FAR_FIRST_8:
        hp, lp = z_at(d)
        send(r.b3s.at[hp], r.b3r.at[d - 1], r.rs_s.at[1, 2], r.rs_r.at[1, 2], zh=hp, zl=lp)

    take_bytes(r.c2r, r.rs_r.at[2, 1])
    total = r.c2s[y].astype(F32)
    for d in range(7):
        total = total + r.c2r[d].astype(F32)
    r.c3s[...] = total.astype(BF)
    for d in FAR_FIRST_4:
        xp = turned(x, d, 4)
        send(r.c3s, r.c3r.at[d - 1], r.rs_s.at[2, 2], r.rs_r.at[2, 2], x=xp)

    value_scores(3)
    state_third(1)

    vg_whole = jnp.concatenate([r.vg[0], r.vg[1]], axis=1)

    for n in range(8):
        rows = r.wb[pl.ds(n * 4, 4)].reshape(256, KV_WIDTH)
        col = span(n * 256, 256)
        r.igo[:, col] = dot(vg_whole, rows, ((1,), (1,))).astype(BF)


    factor = 1.0 / math.sqrt(TOKEN_COUNT)
    here_x, here_zl = c * 4 + x, c * 4 + zl

    def spread(src, dst, part, axis, at):
        target = 0 if part == 0 else 1
        for d in FAR_FIRST_4:
            where = {axis: turned(at, d, 4), "c": target}
            send(src, dst, r.rs_s.at[part, 3], r.rs_r.at[part, 3], **where)

        @pl.when(c != target)
        def _():
            send(src, dst, r.rs_s.at[part, 3], r.rs_r.at[part, 3], c=target)

    take_bytes(r.a3r, r.rs_r.at[0, 2])
    total = r.a3s[zh].astype(F32)
    for d in range(7):
        total = total + r.a3r[d].astype(F32)
    r.fa[...] = total * factor
    spread(r.fa, r.wga.at[here_x], 0, "x", x)
    take_bytes(r.c3r, r.rs_r.at[2, 2])
    total = r.c3s[...].astype(F32)
    for d in range(3):
        total = total + r.c3r[d].astype(F32)
    r.fc[...] = total * factor
    spread(r.fc, r.wgc.at[here_zl], 2, "zl", zl)
    take_bytes(r.b3r, r.rs_r.at[1, 2])
    total = r.b3s[zh].astype(F32)
    for d in range(7):
        total = total + r.b3r[d].astype(F32)
    r.fb[...] = total * factor
    spread(r.fb, r.wgb.at[here_x], 1, "x", x)

    state_wait(1)

    for p in range(4):
        pair = r.st_r3[1, p].astype(F32)
        other_way = pltpu.roll(pair, 64, 1)
        for g in range(2):
            low, high = (pair, other_way) if g == 0 else (other_way, pair)
            block = jnp.concatenate(
                [jnp.where(low64, low, 0.0), jnp.where(low64, 0.0, high)], axis=0
            ).astype(BF)
            for j in range(2):
                col = span(p * 512 + g * 256 + j * 128, 128)
                r.qgo[:, col] = (r.qgi[:, col] + dot(r.s[:, col], block)).astype(BF)


    @pl.when(c == 0)
    def _():
        r.wga[here_x] = r.fa[...]
        take_bytes(r.wga.at[pl.ds(0, 7)], r.rs_r.at[0, 3])
        for n in range(8):
            cp, u = divmod(n, 4)
            r.wgo[16 * u : 16 * u + 16, 256 * cp : 256 * cp + 256] = r.wga[n]
        take_bytes(r.wga.at[pl.ds(0, 3)], r.rs_s.at[0, 3])
        take_bytes(r.wgb.at[pl.ds(0, 4)], r.rs_s.at[1, 3])
        take_bytes(r.wgc.at[pl.ds(0, 4)], r.rs_s.at[2, 3])

    @pl.when(c == 1)
    def _():
        r.wgb[here_x] = r.fb[...]
        r.wgc[here_zl] = r.fc[...]
        take_bytes(r.wgb.at[pl.ds(0, 7)], r.rs_r.at[1, 3])
        take_bytes(r.wgc.at[pl.ds(0, 7)], r.rs_r.at[2, 3])
        for n in range(8):
            cp, u = divmod(n, 4)
            r.wgo[16 * u : 16 * u + 16, 256 * cp : 256 * cp + 128] = r.wgb[n]
            r.wgo[16 * u : 16 * u + 16, 256 * cp + 128 : 256 * cp + 256] = r.wgc[n]
        take_bytes(r.wga.at[pl.ds(0, 4)], r.rs_s.at[0, 3])
        take_bytes(r.wgb.at[pl.ds(0, 3)], r.rs_s.at[1, 3])
        take_bytes(r.wgc.at[pl.ds(0, 3)], r.rs_s.at[2, 3])


    take_bytes(r.wb.at[pl.ds(0, 16)], r.wd_s.at[0])

    @pl.when((zl == 0) | (zl == 3))
    def _():
        take_bytes(r.wb.at[pl.ds(0, 2)], r.wz_s.at[0])

    take_bytes(r.wb.at[pl.ds(0, 14)], r.wr_s.at[0])
    take_bytes(r.x, r.xx_s.at[0])
    take_bytes(r.vgp, r.vv_s.at[0])
    for i in range(2):
        take_bytes(r.st_s.at[i, pl.ds(0, 3)], r.st_ss.at[i, 0])
        take_bytes(row_sums[i].at[pl.ds(0, 3)], r.st_ss.at[i, 1])
        take_bytes(r.st_o.at[i, pl.ds(0, 3)], r.st_ss.at[i, 2])
    sent = [
        [r.a1, r.a2r, r.a3r],
        [r.b1, r.b2r, r.b3r],
        [r.c1, r.c2r, r.c3r],
    ]
    for part in range(3):
        for n in range(3):
            take_bytes(sent[part][n], r.rs_s.at[part, n])


def put_out(*refs):
    copies = [
        pltpu.make_async_copy(refs[i], refs[i + 4], refs[8].at[i]) for i in range(4)
    ]
    for copy in copies:
        copy.start()
    for copy in copies:
        copy.wait()


def body(inputs, queries, keys, value_matrix, out_grad):
    anywhere = pl.BlockSpec(memory_space=pl.ANY)
    in_vmem = pl.BlockSpec(memory_space=pltpu.VMEM)
    results = pl.pallas_call(
        kernel,
        out_shape=tuple(jax.ShapeDtypeStruct(*spec) for spec in OUTS.values()),
        in_specs=[pl.BlockSpec(memory_space=pltpu.HBM)] * 5,
        out_specs=(in_vmem,) * 4,
        scratch_shapes=[pltpu.VMEM(*spec) for spec in VMEM_SCRATCH.values()]
        + [pltpu.SemaphoreType.DMA(shape) for shape in SEM_SCRATCH.values()],
        compiler_params=pltpu.CompilerParams(
            collective_id=0, has_side_effects=True, vmem_limit_bytes=40 << 20
        ),
    )(
        *(
            pltpu.with_memory_space_constraint(a, pltpu.HBM)
            for a in (inputs[0], queries[0], keys[0], value_matrix, out_grad[0])
        )
    )
    query_gradient, key_gradient, input_grad, weight_grad = pl.pallas_call(
        put_out,
        out_shape=tuple(jax.ShapeDtypeStruct(*spec) for spec in OUTS.values()),
        in_specs=[in_vmem] * 4,
        out_specs=(anywhere,) * 4,
        scratch_shapes=[pltpu.SemaphoreType.DMA((4,))],
        compiler_params=pltpu.CompilerParams(vmem_limit_bytes=8 << 20),
    )(*results)
    return query_gradient[None], key_gradient[None], input_grad[None], weight_grad


def solution(mesh):
    torus = Mesh(mesh.devices.reshape(4, 4, 2, 8, 2), AXES)
    wide = P(DP, SEQ, None)
    return jax.shard_map(
        body,
        mesh=torus,
        in_specs=(wide, wide, wide, P(DP, None), wide),
        out_specs=(wide, wide, wide, P(DP, None)),
        check_vma=False,
    )
```
